128 devices in a mesh: wide: 32 (over z, x, core), narrow: 4 (over y).
Axes of the slice: x: 4, y: 4, z: 4, core: 2. Of those that a mesh axis runs over, the one named last changes fastest.
Arguments:
- dens_tiles: bfloat16 [2048, 3, 128, 128], P(('wide', 'narrow')), may hold values from -6 to 6
- tile_dest: int32 [2048, 2], P(('wide', 'narrow')), may hold values from 0 to 31, all different within a row; in each aligned block of 16 rows (0 to 15, 16 to 31, ...) at most 2 rows name the same one
- tile_place: int32 [2048, 2], P(('wide', 'narrow')), may hold values from 0 to 49
- tile_rows: int32 [2048], P(('wide', 'narrow')), may hold values from 0 to 3
- tile_cols: int32 [2048], P(('wide', 'narrow')), may hold values from 0 to 31
- ao_values: bfloat16 [64, 640, 1280], P('wide'), may hold values from -0.25 to 0.25
- point_count: int32 [64], P('wide'), may hold values from 1 to 1280, 51200 in all
- weights: float32 [64, 1280], P('wide'), may hold values from 0.05 to 1
- kernel_first: float32 [64, 1280], P('wide'), may hold values from -1.5 to -0.3
- kernel_second: float32 [64, 1280], P('wide'), may hold values from 0.2 to 2
- occ_coef: bfloat16 [16384, 512], P('wide'), may hold values from -0.3125 to 0.3125
- vir_coef: bfloat16 [16384, 1024], P('narrow'), may hold values from -0.3125 to 0.3125
Outputs:
- response: float32 [3, 512, 1024], P(None, 'wide', 'narrow')
The draws below stay inside these ranges and needn't reach their ends.
Inputs may be any that keep to these rules, and one draw needn't show every extreme that they name: `tile_dest`: among the routes of one device's 16 tiles, no wide index is named more than 2 times, and some device names some index exactly 2 times; the 2 indices of one tile differ. `point_count`: the counts of all batches sum to 51200.
All inputs are finite; a program needn't handle non-finite values. No bound on the sum of `point_count` on one device may be relied on, other than what follows from the above.
Results may differ from the reference program's by a relative error of at most 0.0074.
Values may be sent and summed in bfloat16 or wider, within the bound.
A program may use at most 128 MiB of HBM per device.

```python
import math
import jax
import jax.numpy as jnp
import numpy as np
from jax import lax

NAO = 16384
NOCC = 512
NVIR = 1024
BLK = 128
KB = 5
FIELDS = 3
TOP = 2
TILE_DEV = 16
NBAT = 2
PTS = 1280
RB = 4
CB = 32
CAP = 2
TILES = 2048
BATCHES = 64
N_WIDE = 32
N_NARROW = 4
DEVICES = 128


def place_ends(drawn, stream_key, least, high):
    index_at = [jax.random.randint(jax.random.fold_in(stream_key, axis), (), 0, length) for axis, length in enumerate(drawn.shape)]
    longest = drawn.shape.index(max(drawn.shape))
    beside = index_at[:longest] + [(index_at[longest] + 1) % drawn.shape[longest]] + index_at[longest + 1:]
    return drawn.at[tuple(index_at)].set(least).at[tuple(beside)].set(high)


def shard_levels(stream_key, dims, cuts, low, largest):
    level, own = 1.0, jax.random.fold_in(stream_key, 6)
    for position, shards_of in cuts:
        heights = jnp.exp(jax.random.uniform(jax.random.fold_in(own, position), (shards_of,), jnp.float32, low / len(cuts), largest / len(cuts)))
        level = level * jnp.repeat(heights, dims[position] // shards_of).reshape([-1 if axis == position else 1 for axis in range(len(dims))])
    return level


def profile(amount, total, reach, lean):
    weights = [(1 << 20) // math.isqrt(standing ** lean) + 1 for standing in range(2, amount + 1)]
    spare, counts = total - reach - (amount - 1), [1] * (amount - 1)
    while spare > 0:
        free = [i for i in range(amount - 1) if counts[i] < reach]
        whole, budget = sum([weights[i] for i in free]), spare
        for i in free:
            more = min(reach - counts[i], max(1, budget * weights[i] // whole), spare)
            counts[i] = counts[i] + more
            spare = spare - more
    return np.array([reach] + counts)


def ragged_sizes(own_key, count, total, bound, slope):
    if count == 2:
        one = jax.random.randint(own_key, (), max(1, total - bound), min(bound, total - 1) + 1)
        return jnp.stack([one, total - one])
    lengths = jnp.asarray(profile(count, total, bound, slope), jnp.int32)
    pairs = (count - 1) // 2
    donor, receiver = lengths[1:1 + 2 * pairs:2], lengths[2:2 + 2 * pairs:2]
    slack = jnp.minimum(donor - 1, bound - receiver)
    moved = jax.random.randint(jax.random.fold_in(own_key, 1), (pairs,), 0, 1 << 20) % (slack + 1)
    lengths = lengths.at[1:1 + 2 * pairs:2].set(donor - moved).at[2:2 + 2 * pairs:2].set(receiver + moved)
    return lengths[jax.random.permutation(jax.random.fold_in(own_key, 2), count)]


def routed_block(stream_key, own, number, rows, number_of, top, limit, lean):
    sequence = jax.random.permutation(stream_key, number_of)
    packed, ordinary = portions_of(number_of, rows * top, limit, lean, True), portions_of(number_of, rows * top, limit, lean, False)
    places = jnp.arange(number_of)

    def named(sizes, rotation):
        used = int((sizes > 0).sum())
        fixed = max(1, used // 4)
        moved = fixed + (places - fixed + rotation * (used - fixed)) % max(1, number_of - fixed)
        return jnp.zeros((number_of,), jnp.int32).at[sequence[jnp.where(places < fixed, places, moved)]].set(jnp.asarray(sizes, jnp.int32))

    sizes = jnp.where(number % 4 == 0, named(packed, number // 4), named(ordinary, number - number // 4 - 1))
    mixed = jax.random.permutation(jax.random.fold_in(own, 3), number_of)
    donor, receiver = mixed[0:number_of // 2 * 2:2], mixed[1:number_of // 2 * 2:2]
    slack = jnp.minimum(sizes[donor] - 1, limit - sizes[receiver]) // 2
    slack = jnp.where((donor == sequence[0]) | (receiver == sequence[0]) | (sizes[receiver] == 0), 0, jnp.maximum(slack, 0))
    moved = jax.random.randint(jax.random.fold_in(own, 4), (number_of // 2,), 0, 1 << 20) % (slack + 1)
    sizes = sizes.at[donor].add(-moved).at[receiver].add(moved)
    labels = jnp.searchsorted(jnp.cumsum(sizes), jnp.arange(rows * top), side="right").astype(jnp.int32)
    listing = labels.reshape(top, rows).T
    listing = listing[jax.random.permutation(jax.random.fold_in(own, 1), rows)]
    rotation = jax.random.randint(jax.random.fold_in(own, 2), (rows, 1), 0, top)
    return jnp.take_along_axis(listing, (jnp.arange(top)[None, :] + rotation) % top, axis=1)


def portions_of(amount, total, reach, skew, full):
    weights = [(1 << 20) // math.isqrt(rank ** skew) + 1 for rank in range(1, amount + 1)]
    largest = reach if full else min(reach, max(-(-total // amount), total * weights[0] // sum(weights)))
    least = 1 if total - largest >= amount - 1 else 0
    counts, spare = [largest] + [least] * (amount - 1), total - largest - least * (amount - 1)
    while spare > 0:
        free = [i for i in range(1, amount) if counts[i] < largest] or [i for i in range(1, amount) if counts[i] < reach]
        mass, left = sum([weights[i] for i in free]), spare
        for i in free:
            addition = min(reach - counts[i], max(1, left * weights[i] // mass), spare)
            counts[i] = counts[i] + addition
            spare = spare - addition
    return np.array(counts)


def scatter_about(key, shape, scale, reach, cuts=(), kind=jnp.bfloat16):
    entries = scale * jax.random.normal(key, shape, jnp.float32)
    if cuts:
        entries = entries * shard_levels(key, shape, cuts, -0.22, 0.18)
    return jnp.clip(entries, -reach, reach).astype(kind)


def setup_inputs(seed: int = 0) -> dict:
    key_list = jax.random.split(jax.random.key(seed), 13)
    dens_tiles = scatter_about(key_list[0], (TILES, FIELDS, BLK, BLK), 1.0, 6.0, ((0, 128),))
    tile_dest_keys = jax.random.split(jax.random.fold_in(key_list[1], 1), TILES // TILE_DEV)
    tile_dest_turns = jax.random.permutation(jax.random.fold_in(key_list[1], 3), TILES // TILE_DEV)
    tile_dest = jax.vmap(lambda own, number: routed_block(jax.random.fold_in(key_list[1], 2), own, number, TILE_DEV, N_WIDE, TOP, CAP, 2))(tile_dest_keys, tile_dest_turns).reshape((TILES, TOP))
    tile_place = place_ends(jax.random.randint(key_list[2], (TILES, TOP), 0, NBAT * KB * KB), jax.random.fold_in(key_list[2], 1), 0, (NBAT * KB * KB) - 1).astype(jnp.int32)
    tile_rows = place_ends(jax.random.randint(key_list[3], (TILES,), 0, RB), jax.random.fold_in(key_list[3], 1), 0, RB - 1).astype(jnp.int32)
    tile_cols = place_ends(jax.random.randint(key_list[4], (TILES,), 0, CB), jax.random.fold_in(key_list[4], 1), 0, CB - 1).astype(jnp.int32)
    ao_values = scatter_about(key_list[5], (BATCHES, KB * BLK, PTS), (KB * BLK) ** -0.5, 0.25, ((0, 32),))
    point_count = ragged_sizes(key_list[6], BATCHES, BATCHES * PTS * 5 // 8, PTS, 2).astype(jnp.int32)
    weights = jnp.clip(jnp.exp(math.log(1.0) - 2.9957323 * jax.random.uniform(key_list[7], (BATCHES, PTS), jnp.float32) ** shard_levels(key_list[7], (BATCHES, PTS), ((0, 32),), -0.2, 0.2)), 0.05, 1.0)
    kernel_first = jnp.clip(-1.5 + 1.2 * jax.random.uniform(key_list[8], (BATCHES, PTS), jnp.float32) ** shard_levels(key_list[8], (BATCHES, PTS), ((0, 32),), -0.2, 0.2), -1.5, -0.3)
    kernel_second = jnp.clip(0.2 + 1.8 * jax.random.uniform(key_list[9], (BATCHES, PTS), jnp.float32) ** shard_levels(key_list[9], (BATCHES, PTS), ((0, 32),), -0.2, 0.2), 0.2, 2.0)
    occ_coef = scatter_about(key_list[10], (NAO, NOCC), (3 * BLK) ** -0.5, 0.3125, ((0, 32),))
    vir_coef = scatter_about(key_list[11], (NAO, NVIR), (3 * BLK) ** -0.5, 0.3125, ((0, 4),))
    return dict(dens_tiles=dens_tiles, tile_dest=tile_dest, tile_place=tile_place, tile_rows=tile_rows, tile_cols=tile_cols, ao_values=ao_values, point_count=point_count, weights=weights, kernel_first=kernel_first, kernel_second=kernel_second, occ_coef=occ_coef, vir_coef=vir_coef)


def field_potential(density, kernel_one, kernel_two, point_scale):
    dens_a = density[:, 0]
    dens_b = density[:, 1]
    dens_c = density[:, 2]
    stacked = jnp.stack([kernel_one * dens_a + kernel_two * dens_b * dens_c,
                         kernel_one * dens_b + kernel_two * dens_a * dens_c,
                         kernel_one * dens_c + kernel_two * dens_a * dens_b], axis=1)
    return stacked * point_scale[:, None, :]


def reference(dens_tiles, tile_dest, tile_place, tile_rows, tile_cols, ao_values, point_count, weights, kernel_first, kernel_second, occ_coef, vir_coef):
    batch_slots = NBAT * KB * KB
    tile_len = FIELDS * BLK * BLK
    ao_width = KB * BLK
    flat_tiles = dens_tiles.reshape(TILES, tile_len).astype(jnp.float32)
    narrow_of = ((jnp.arange(TILES) // TILE_DEV) % N_NARROW).astype(jnp.int32)
    trash = N_NARROW * batch_slots
    ao_all = ao_values.reshape(N_WIDE, NBAT, ao_width, PTS)
    inside = jnp.arange(PTS)[None, :] < point_count[:, None]
    scale_all = jnp.where(inside, weights, jnp.float32(0.0)).reshape(N_WIDE, NBAT, PTS)
    first_all = kernel_first.reshape(N_WIDE, NBAT, PTS)
    second_all = kernel_second.reshape(N_WIDE, NBAT, PTS)

    def receive(wide_idx):
        land_grid = jnp.zeros((trash + 1, tile_len), jnp.float32)
        for route in range(TOP):
            seg_ids = jnp.where(tile_dest[:, route] == wide_idx, narrow_of * batch_slots + tile_place[:, route], trash).astype(jnp.int32)
            land_grid = land_grid + jax.ops.segment_sum(flat_tiles, seg_ids, num_segments=trash + 1)
        land_grid = land_grid[:trash].astype(jnp.bfloat16)
        dens_grid = land_grid.reshape(N_NARROW, NBAT, KB, KB, FIELDS, BLK, BLK).transpose(0, 1, 4, 2, 5, 3, 6)
        dens_grid = dens_grid.reshape(N_NARROW, NBAT, FIELDS, ao_width, ao_width)
        ao_float = lax.dynamic_index_in_dim(ao_all, wide_idx, 0, keepdims=False).astype(jnp.float32)
        mixed_rows = jnp.einsum('cbfmn,bnp->cbfmp', dens_grid.astype(jnp.float32), ao_float)
        density = jnp.sum(jnp.sum(mixed_rows * ao_float[None, :, None], axis=3), axis=0)
        point_scale = lax.dynamic_index_in_dim(scale_all, wide_idx, 0, keepdims=False)
        kernel_one = lax.dynamic_index_in_dim(first_all, wide_idx, 0, keepdims=False)
        kernel_two = lax.dynamic_index_in_dim(second_all, wide_idx, 0, keepdims=False)
        potential = field_potential(density, kernel_one, kernel_two, point_scale)
        scaled = (ao_float[:, None] * potential[:, :, None, :]).astype(jnp.bfloat16)
        blocks = jnp.einsum('bfmp,bnp->bfmn', scaled.astype(jnp.float32), ao_float)
        blocks = blocks.reshape(NBAT, FIELDS, KB, BLK, KB, BLK).transpose(0, 2, 4, 1, 3, 5)
        return blocks.reshape(batch_slots, tile_len).astype(jnp.bfloat16)

    answers = lax.map(receive, jnp.arange(N_WIDE, dtype=jnp.int32))
    tile_potential = jnp.zeros((TILES, tile_len), jnp.float32)
    for route in range(TOP):
        tile_potential = tile_potential + answers[tile_dest[:, route], tile_place[:, route]].astype(jnp.float32)
    tile_potential = tile_potential.astype(jnp.bfloat16).reshape(DEVICES, TILE_DEV, FIELDS, BLK, BLK)
    occ_blocks = occ_coef.reshape(NAO // BLK, BLK, NOCC)
    vir_blocks = vir_coef.reshape(NAO // BLK, BLK, NVIR)
    rows_dev = tile_rows.reshape(DEVICES, TILE_DEV)
    cols_dev = tile_cols.reshape(DEVICES, TILE_DEV)

    def project(summed, carried):
        device, pieces, occ_rows, vir_cols = carried
        wide_idx = device // N_NARROW
        narrow_idx = device % N_NARROW
        occ_sel = occ_blocks[wide_idx * RB + occ_rows].astype(jnp.float32)
        vir_sel = vir_blocks[narrow_idx * CB + vir_cols].reshape(TILE_DEV * BLK, NVIR)
        left_half = jnp.einsum('tao,tfab->fotb', occ_sel, pieces.astype(jnp.float32)).astype(jnp.bfloat16)
        term = jnp.dot(left_half.reshape(FIELDS * NOCC, TILE_DEV * BLK), vir_sel, preferred_element_type=jnp.float32)
        return summed + term.reshape(FIELDS, NOCC, NVIR), None

    start = jnp.zeros((FIELDS, NOCC, NVIR), jnp.float32)
    response, _ = lax.scan(project, start, (jnp.arange(DEVICES, dtype=jnp.int32), tile_potential, rows_dev, cols_dev))
    return response
```

```python
import jax
import jax.numpy as jnp
from jax import lax
from jax.experimental import pallas as pl
from jax.experimental.pallas import tpu as pltpu
from jax.sharding import PartitionSpec as P

NOCC = 512
NVIR = 1024
BLK = 128
KB = 5
FIELDS = 3
NBAT = 2
PTS = 1280
SIDE = 4
NWIDE = 32
ROWS = FIELDS * BLK
MESH = pl.DeviceIdType.MESH
CHIPS = [(2, 2), (1, 1), (3, 3), (1, 3), (3, 1), (1, 2), (3, 2), (2, 1), (2, 3), (0, 2), (2, 0), (0, 1), (0, 3), (1, 0), (3, 0)]
OFFSETS = [(z, x, c) for z, x in CHIPS for c in range(2)] + [(0, 0, 1)]


def shifted(me, offset, sign=1):
    z, x, c = me // 8, (me // 2) % 4, me % 2
    z = (z + sign * offset[0] + 2 * SIDE) % SIDE
    x = (x + sign * offset[1] + 2 * SIDE) % SIDE
    c = (c + offset[2]) % 2
    return z * 8 + x * 2 + c


def number(offset):
    return offset[0] * 8 + offset[1] * 2 + offset[2]


def dispatch_kernel(
    sel_ref, meta_ref, tiles_ref, ao_ref, dens_ref, info_ref,
    outb, inb, acc, mine, parts,
    send_sem, recv_sem, meta_send, meta_recv, part_send, part_recv,
):
    me = lax.axis_index("wide")
    row = lax.axis_index("narrow")
    barrier = pltpu.get_barrier_semaphore()
    for offset in OFFSETS:
        pl.semaphore_signal(
            barrier, inc=1, device_id={"wide": shifted(me, offset)}, device_id_type=MESH
        )
    for step in range(1, SIDE):
        pl.semaphore_signal(
            barrier, inc=1, device_id={"narrow": (row + step) % SIDE}, device_id_type=MESH
        )

    def build(i, carry):
        outb[i] = tiles_ref[sel_ref[i]]
        return carry

    lax.fori_loop(0, 2 * NWIDE, build, 0)
    acc[...] = jnp.zeros_like(acc)
    pl.semaphore_wait(barrier, len(OFFSETS) + SIDE - 1)

    sent = []

    def send(src, dst, ssem, rsem, peer):
        copy = pltpu.make_async_remote_copy(
            src_ref=src, dst_ref=dst, send_sem=ssem, recv_sem=rsem,
            device_id={"wide": peer}, device_id_type=MESH,
        )
        copy.start()
        sent.append(copy)

    for offset in OFFSETS:
        peer, k = shifted(me, offset), number(offset)
        send(meta_ref.at[peer], info_ref.at[me], meta_send.at[k], meta_recv.at[k], peer)
    info_ref[me] = meta_ref[me]
    for offset in OFFSETS:
        peer, k = shifted(me, offset), number(offset)
        for j in range(2):
            send(
                outb.at[2 * peer + j], inb.at[2 * me + j], send_sem.at[k, j], recv_sem.at[k, j], peer
            )

    def use(tile, code):
        first, second = code % 16, (code // 16) % 16
        batch, valid = (code // 256) % 2, (code // 32768) % 2
        lives = [jnp.logical_and(valid == 1, batch == b) for b in range(NBAT)]
        for q in range(PTS // 256):
            cols = pl.ds(q * 256, 256)
            mixed = jnp.dot(tile, ao_ref[second, :, cols], preferred_element_type=jnp.float32)
            left = ao_ref[first, :, cols].astype(jnp.float32)
            part = jnp.sum(
                mixed.reshape(FIELDS, BLK // 8, 8, 256) * left.reshape(1, BLK // 8, 8, 256), axis=1
            )
            for b in range(NBAT):
                acc[b, :, :, cols] += jnp.where(lives[b], part, 0.0)

    def code_of(ref, source, j):
        return ref[source, 0:1, j : j + 1][0, 0]

    for j in range(2):
        use(outb[2 * me + j], code_of(meta_ref, me, j))

    for offset in OFFSETS:
        peer, k = shifted(me, offset), number(offset)
        pltpu.make_async_remote_copy(
            src_ref=meta_ref.at[0], dst_ref=info_ref.at[0], send_sem=meta_send.at[k],
            recv_sem=meta_recv.at[k], device_id={"wide": peer}, device_id_type=MESH,
        ).wait_recv()

    def take(offset):
        k, source = number(offset), shifted(me, offset, -1)
        for j in range(2):
            pltpu.make_async_remote_copy(
                src_ref=outb.at[0], dst_ref=inb.at[2 * source + j], send_sem=send_sem.at[k, j],
                recv_sem=recv_sem.at[k, j], device_id={"wide": source}, device_id_type=MESH,
            ).wait_recv()
            use(inb[2 * source + j], code_of(info_ref, source, j))

    take((0, 0, 1))

    def arrive(i, carry):
        chip = i // 2
        dz = sum(jnp.where(chip == n, z, 0) for n, (z, _) in enumerate(CHIPS))
        dx = sum(jnp.where(chip == n, x, 0) for n, (_, x) in enumerate(CHIPS))
        take((dz, dx, i % 2))
        return carry

    lax.fori_loop(0, 2 * len(CHIPS), arrive, 0)

    for b in range(NBAT):
        for f in range(FIELDS):
            mine[pl.ds(b * FIELDS + f, 1), :] = jnp.sum(acc[b, f], axis=0, keepdims=True)
    mine[pl.ds(6, 2), :] = jnp.zeros((2, PTS), jnp.float32)
    total = mine[...]
    swaps = []
    for step in range(1, SIDE):
        copy = pltpu.make_async_remote_copy(
            src_ref=mine, dst_ref=parts.at[step - 1], send_sem=part_send.at[step - 1],
            recv_sem=part_recv.at[step - 1], device_id={"narrow": (row + step) % SIDE},
            device_id_type=MESH,
        )
        copy.start()
        swaps.append(copy)
    for copy in sent:
        copy.wait_send()
    for step, copy in enumerate(swaps):
        copy.wait()
        total = total + parts[step]
    dens_ref[...] = total


def dispatch(sel, meta, tiles, ao):
    vmem, smem = pl.BlockSpec(memory_space=pltpu.VMEM), pl.BlockSpec(memory_space=pltpu.SMEM)
    dma = pltpu.SemaphoreType.DMA
    return pl.pallas_call(
        dispatch_kernel,
        out_shape=(
            jax.ShapeDtypeStruct((8, PTS), jnp.float32),
            jax.ShapeDtypeStruct((NWIDE, 8, BLK), jnp.int32),
        ),
        in_specs=[smem, vmem, vmem, vmem],
        out_specs=(vmem, vmem),
        scratch_shapes=[
            pltpu.VMEM((2 * NWIDE, ROWS, BLK), jnp.bfloat16),
            pltpu.VMEM((2 * NWIDE, ROWS, BLK), jnp.bfloat16),
            pltpu.VMEM((NBAT, FIELDS, 8, PTS), jnp.float32),
            pltpu.VMEM((8, PTS), jnp.float32),
            pltpu.VMEM((SIDE - 1, 8, PTS), jnp.float32),
            dma((NWIDE, 2)), dma((NWIDE, 2)),
            dma((NWIDE,)), dma((NWIDE,)), dma((SIDE - 1,)), dma((SIDE - 1,)),
        ],
        compiler_params=pltpu.CompilerParams(
            collective_id=0, has_side_effects=True, vmem_limit_bytes=30 * 2**20
        ),
        cost_estimate=pl.CostEstimate(
            flops=70_000_000_000, bytes_accessed=10_000_000, transcendentals=0
        ),
    )(sel, meta, tiles, ao)


def respond_kernel(
    code_ref, count_ref, dens_ref, weight_ref, first_ref, second_ref, ao_ref, occ_hbm, vir_hbm,
    out_ref, occ, vir, pot, scaled, answer, total, left, head, follow, occ_sem, vir_sem,
):
    load_occ = pltpu.make_async_copy(occ_hbm, occ, occ_sem)
    load_vir = pltpu.make_async_copy(vir_hbm, vir, vir_sem)
    load_occ.start()
    load_vir.start()

    lane = lax.broadcasted_iota(jnp.int32, (1, PTS), 1)
    for b in range(NBAT):
        scale = jnp.where(lane < count_ref[b], weight_ref[pl.ds(b, 1), :], 0.0)
        one, two = first_ref[pl.ds(b, 1), :], second_ref[pl.ds(b, 1), :]
        d = [dens_ref[pl.ds(b * FIELDS + f, 1), :] for f in range(FIELDS)]
        for f in range(FIELDS):
            p, q = d[(f + 1) % 3], d[(f + 2) % 3]
            pot[pl.ds(b * FIELDS + f, 1), :] = scale * (one * d[f] + two * p * q)

    def blocks(i, carry):
        b, f = i // FIELDS, i % FIELDS
        aos = ao_ref[pl.ds(b * KB, KB)].reshape(KB * BLK, PTS)
        scaled[...] = (aos.astype(jnp.float32) * pot[pl.ds(i, 1), :]).astype(jnp.bfloat16)
        part = lax.dot_general(
            scaled[...], aos, (((1,), (1,)), ((), ())), preferred_element_type=jnp.float32
        ).astype(jnp.bfloat16)
        for a in range(KB):
            for c in range(KB):
                answer[b * 25 + a * KB + c, :, pl.ds(pl.multiple_of(f * BLK, BLK), BLK)] = part[
                    a * BLK : (a + 1) * BLK, c * BLK : (c + 1) * BLK
                ]
        return carry

    lax.fori_loop(0, NBAT * FIELDS, blocks, 0)

    def clear(c, carry):
        head[c] = -1
        return carry

    lax.fori_loop(0, 32, clear, 0)

    def link(r, carry):
        code = code_ref[r]
        column = (code // 262144) % 32

        @pl.when((code // 32768) % 2 == 1)
        def _():
            follow[r] = head[column]
            head[column] = r

        return carry

    lax.fori_loop(0, 2 * NWIDE, link, 0)
    load_occ.wait()

    def column_sum(c, carry):
        total[...] = jnp.zeros_like(total)

        def add(r):
            code = code_ref[r]
            block = (r // 2) * 4 + (code // 65536) % 4
            total[...] += jnp.dot(
                occ[block], answer[(code // 512) % 64], preferred_element_type=jnp.float32
            )
            return follow[r]

        lax.while_loop(lambda r: r >= 0, add, head[c])
        for f in range(FIELDS):
            left[pl.ds(f * NOCC, NOCC), pl.ds(pl.multiple_of(c * BLK, BLK), BLK)] = total[
                :, f * BLK : (f + 1) * BLK
            ].astype(jnp.bfloat16)
        return carry

    lax.fori_loop(0, 32, column_sum, 0)
    load_vir.wait()

    def project(i, carry):
        q, f = i // FIELDS, i % FIELDS
        rows = pl.ds(pl.multiple_of(f * NOCC, NOCC), NOCC)
        out_ref[q, rows, :] = jnp.dot(
            left[rows, :], vir[:, pl.ds(pl.multiple_of(q * 256, 256), 256)],
            preferred_element_type=jnp.float32,
        ).astype(jnp.bfloat16)
        return carry

    lax.fori_loop(0, SIDE * FIELDS, project, 0)


def respond(codes, counts, dens, weights, first, second, ao, occ, vir):
    vmem, smem = pl.BlockSpec(memory_space=pltpu.VMEM), pl.BlockSpec(memory_space=pltpu.SMEM)
    hbm = pl.BlockSpec(memory_space=pl.ANY)
    return pl.pallas_call(
        respond_kernel,
        out_shape=jax.ShapeDtypeStruct((SIDE, FIELDS * NOCC, 256), jnp.bfloat16),
        in_specs=[smem, smem, vmem, vmem, vmem, vmem, vmem, hbm, hbm],
        out_specs=vmem,
        scratch_shapes=[
            pltpu.VMEM((128, NOCC, BLK), jnp.bfloat16),
            pltpu.VMEM((4096, NVIR), jnp.bfloat16),
            pltpu.VMEM((8, PTS), jnp.float32),
            pltpu.VMEM((KB * BLK, PTS), jnp.bfloat16),
            pltpu.VMEM((50, BLK, ROWS), jnp.bfloat16),
            pltpu.VMEM((NOCC, ROWS), jnp.float32),
            pltpu.VMEM((FIELDS * NOCC, 4096), jnp.bfloat16),
            pltpu.SMEM((32,), jnp.int32),
            pltpu.SMEM((64,), jnp.int32),
            pltpu.SemaphoreType.DMA,
            pltpu.SemaphoreType.DMA,
        ],
        compiler_params=pltpu.CompilerParams(vmem_limit_bytes=62 * 2**20),
        cost_estimate=pl.CostEstimate(
            flops=30_000_000_000, bytes_accessed=30_000_000, transcendentals=0
        ),
    )(codes, counts, dens, weights, first, second, ao, occ, vir)


def turn_kernel(occ_ref, out_ref):
    row = lax.axis_index("narrow")
    out_ref[...] = occ_ref[pl.ds(pl.multiple_of(row * BLK, BLK), BLK), :].T


def turned(occ):
    vmem = pl.BlockSpec(memory_space=pltpu.VMEM)
    return pl.pallas_call(
        turn_kernel, out_shape=jax.ShapeDtypeStruct((NOCC, BLK), occ.dtype), in_specs=[vmem],
        out_specs=vmem,
    )(occ)


def body(
    dens_tiles,
    tile_dest,
    tile_place,
    tile_rows,
    tile_cols,
    ao_values,
    point_count,
    weights,
    kernel_first,
    kernel_second,
    occ_coef,
    vir_coef,
):
    tile_count = dens_tiles.shape[0]
    block = turned(occ_coef)
    occ_all = lax.all_gather(block[None], ("wide", "narrow"), axis=0, tiled=True)

    targets = tile_dest.reshape(-1)
    routes = jnp.arange(targets.shape[0])
    earlier = (targets[:, None] == targets[None, :]) & (routes[:, None] > routes[None, :])
    position = targets * 2 + jnp.sum(earlier.astype(jnp.int32), axis=1)
    place = tile_place.reshape(-1)
    batch, slot = place // 25, place % 25
    code = (
        (batch * KB + slot // KB) + 16 * (batch * KB + slot % KB) + 256 * batch + 512 * place + 32768
        + 65536 * jnp.repeat(tile_rows, 2) + 262144 * jnp.repeat(tile_cols, 2)
    )
    chosen = position[None, :] == jnp.arange(2 * NWIDE)[:, None]
    sel = jnp.sum(jnp.where(chosen, routes[None, :] // 2, 0), axis=1)
    codes = jnp.sum(jnp.where(chosen, code[None, :], 0), axis=1)
    meta = jnp.broadcast_to(
        jnp.pad(codes.reshape(NWIDE, 1, 2), ((0, 0), (0, 0), (0, BLK - 2))), (NWIDE, 8, BLK)
    )

    ao = ao_values.reshape(NBAT * KB, BLK, PTS)
    dens, info = dispatch(sel, meta, dens_tiles.reshape(tile_count, ROWS, BLK), ao)
    partial = respond(
        info[:, 0, :2].reshape(-1), point_count, dens, weights, kernel_first, kernel_second, ao,
        occ_all, vir_coef,
    )

    parts = lax.all_to_all(
        partial.reshape(SIDE, FIELDS, NOCC, 256), "narrow", 0, 0, tiled=True
    )
    by_columns = jnp.sum(parts.astype(jnp.float32), axis=0).astype(jnp.bfloat16)
    split = jnp.moveaxis(by_columns.reshape(FIELDS, NWIDE, NOCC // NWIDE, 256), 1, 0)
    owned = lax.all_to_all(split, "wide", 0, 0, tiled=True)
    return jnp.sum(owned.astype(jnp.float32), axis=0)


def solution(mesh):
    in_specs = (
        P(("wide", "narrow"), None, None, None),
        P(("wide", "narrow"), None),
        P(("wide", "narrow"), None),
        P(("wide", "narrow")),
        P(("wide", "narrow")),
        P("wide", None, None),
        P("wide"),
        P("wide", None),
        P("wide", None),
        P("wide", None),
        P("wide", None),
        P("narrow", None),
    )
    out_specs = P(None, "wide", "narrow")
    return jax.shard_map(body, mesh=mesh, in_specs=in_specs, out_specs=out_specs, check_vma=False)
```

```python
import jax
import jax.numpy as jnp
from jax import lax
from jax.experimental import pallas as pl
from jax.experimental.pallas import tpu as pltpu
from jax.sharding import PartitionSpec as P

NOCC = 512
NVIR = 1024
BLK = 128
KB = 5
FIELDS = 3
NBAT = 2
PTS = 1280
SIDE = 4
NWIDE = 32
ROWS = FIELDS * BLK
HALF = FIELDS * NOCC // 2
MESH = pl.DeviceIdType.MESH
CHIPS = [(2, 2), (1, 1), (3, 3), (1, 3), (3, 1), (1, 2), (3, 2), (2, 1), (2, 3), (0, 2), (2, 0), (0, 1), (0, 3), (1, 0), (3, 0)]
BLOCKS_AHEAD, OUT_AHEAD, TILES_AHEAD, ON_AHEAD = 11, 8, 6, 4
OFFSETS = [(z, x, c) for z, x in CHIPS for c in range(2)] + [(0, 0, 1)]


def shifted(me, offset, sign=1):
    z, x, c = me // 8, (me // 2) % 4, me % 2
    z = (z + sign * offset[0] + 2 * SIDE) % SIDE
    x = (x + sign * offset[1] + 2 * SIDE) % SIDE
    c = (c + offset[2]) % 2
    return z * 8 + x * 2 + c


def number(offset):
    return offset[0] * 8 + offset[1] * 2 + offset[2]


def dispatch_kernel(
    sel_ref, meta_ref, tiles_ref, ao_ref, occ_ref, dens_ref, info_ref, all_ref,
    outb, inb, acc, mine, parts, block,
    send_sem, recv_sem, meta_send, meta_recv, part_send, part_recv,
    own_sem, plane_send, plane_recv, side_send, side_recv, pass_send, pass_recv, pair_send, pair_recv,
):
    me = lax.axis_index("wide")
    row = lax.axis_index("narrow")
    barrier = pltpu.get_barrier_semaphore()
    for offset in OFFSETS:
        pl.semaphore_signal(
            barrier, inc=1, device_id={"wide": shifted(me, offset)}, device_id_type=MESH
        )
    for step in range(1, SIDE):
        pl.semaphore_signal(
            barrier, inc=1, device_id={"narrow": (row + step) % SIDE}, device_id_type=MESH
        )

    turned = occ_ref[pl.ds(pl.multiple_of(row * BLK, BLK), BLK), :].T
    for w in range(NWIDE):
        block[pl.ds((w % 2) * 256 + (w // 2) * 16, 16), :] = turned[w * 16 : (w + 1) * 16]

    def build(i, carry):
        outb[i] = tiles_ref[sel_ref[i]]
        return carry

    lax.fori_loop(0, 2 * NWIDE, build, 0)
    acc[...] = jnp.zeros_like(acc)
    pl.semaphore_wait(barrier, len(OFFSETS) + SIDE - 1)

    sent = []

    def send(src, dst, ssem, rsem, peer):
        copy = pltpu.make_async_remote_copy(
            src_ref=src, dst_ref=dst, send_sem=ssem, recv_sem=rsem,
            device_id={"wide": peer}, device_id_type=MESH,
        )
        copy.start()
        sent.append(copy)

    for offset in OFFSETS:
        peer, k = shifted(me, offset), number(offset)
        send(meta_ref.at[peer], info_ref.at[me], meta_send.at[k], meta_recv.at[k], peer)
    info_ref[me] = meta_ref[me]

    def step_of(k):
        dz = sum(jnp.where(k == n + 1, z, 0) for n, (z, _) in enumerate(CHIPS))
        dx = sum(jnp.where(k == n + 1, x, 0) for n, (_, x) in enumerate(CHIPS))
        return dz, dx

    def home_of(k):
        return shifted(me, (*step_of(k), 0), -1)

    def slot(k, c, j, peer, source):
        return pltpu.make_async_remote_copy(
            src_ref=outb.at[2 * peer + j], dst_ref=inb.at[2 * source + j],
            send_sem=send_sem.at[2 * k + c, j], recv_sem=recv_sem.at[2 * k + c, j],
            device_id={"wide": peer}, device_id_type=MESH,
        )

    def send_tiles(k):
        dz, dx = step_of(k)
        for c in range(2):
            for j in range(2):
                slot(k, c, j, shifted(me, (dz, dx, c)), me).start()

    def place(home, y):
        return all_ref.at[home * SIDE + (y + 2 * SIDE) % SIDE]

    def plane(k, peer, home):
        return pltpu.make_async_remote_copy(
            src_ref=block, dst_ref=place(home, row), send_sem=plane_send.at[k],
            recv_sem=plane_recv.at[k], device_id={"wide": peer}, device_id_type=MESH,
        )

    def send_block(k):
        plane(k, shifted(me, (*step_of(k), 0)), me).start()

    def spread(src, k, home, side, way):
        return pltpu.make_async_remote_copy(
            src_ref=src, dst_ref=place(home, row), send_sem=side_send.at[k, side],
            recv_sem=side_recv.at[k, side], device_id={"narrow": (row + way + SIDE) % SIDE},
            device_id_type=MESH,
        )

    def passed(k, home, y, way):
        return pltpu.make_async_remote_copy(
            src_ref=place(home, y), dst_ref=place(home, y), send_sem=pass_send.at[k],
            recv_sem=pass_recv.at[k], device_id={"narrow": (row + way + SIDE) % SIDE},
            device_id_type=MESH,
        )

    def paired(k, home):
        four = all_ref.at[pl.ds(home * SIDE, SIDE)]
        return pltpu.make_async_remote_copy(
            src_ref=four, dst_ref=four, send_sem=pair_send.at[k], recv_sem=pair_recv.at[k],
            device_id={"wide": shifted(me, (0, 0, 1))}, device_id_type=MESH,
        )

    def outward(k):
        home = home_of(k)
        plane(k, home, home).wait_recv()
        for side, way in enumerate((1, -1)):
            spread(place(home, row), k, home, side, way).start()

    def onward(k):
        home = home_of(k)
        for side, way in enumerate((1, -1)):
            pltpu.make_async_remote_copy(
                src_ref=block, dst_ref=place(home, row - way), send_sem=side_send.at[k, side],
                recv_sem=side_recv.at[k, side], device_id={"narrow": (row - way + SIDE) % SIDE},
                device_id_type=MESH,
            ).wait_recv()
        way = 1 - 2 * (k % 2)
        passed(k, home, row - way, way).start()

    def across(k):
        home = home_of(k)
        passed(k, home, row + 2, 1).wait_recv()
        paired(k, home).start()

    def each(first, last, step):
        def run(k, carry):
            step(k)
            return carry

        lax.fori_loop(first, last, run, 0)

    keep = pltpu.make_async_copy(block, place(me, row), own_sem)
    keep.start()
    for side, way in enumerate((1, -1)):
        spread(block, 0, me, side, way).start()
    pair = shifted(me, (0, 0, 1))
    for j in range(2):
        slot(0, 1, j, pair, me).start()
    each(1, 1 + BLOCKS_AHEAD, send_block)
    each(1, 1 + TILES_AHEAD, send_tiles)

    def use(tile, code):
        first, second = code % 16, (code // 16) % 16
        batch, valid = (code // 256) % 2, (code // 32768) % 2
        lives = [jnp.logical_and(valid == 1, batch == b) for b in range(NBAT)]
        for q in range(PTS // 256):
            cols = pl.ds(q * 256, 256)
            mixed = jnp.dot(tile, ao_ref[second, :, cols], preferred_element_type=jnp.float32)
            left = ao_ref[first, :, cols].astype(jnp.float32)
            part = jnp.sum(
                mixed.reshape(FIELDS, BLK // 8, 8, 256) * left.reshape(1, BLK // 8, 8, 256), axis=1
            )
            for b in range(NBAT):
                acc[b, :, :, cols] += jnp.where(lives[b], part, 0.0)

    def code_of(ref, source, j):
        return ref[source, 0:1, j : j + 1][0, 0]

    for j in range(2):
        use(outb[2 * me + j], code_of(meta_ref, me, j))

    for offset in OFFSETS:
        peer, k = shifted(me, offset), number(offset)
        pltpu.make_async_remote_copy(
            src_ref=meta_ref.at[0], dst_ref=info_ref.at[0], send_sem=meta_send.at[k],
            recv_sem=meta_recv.at[k], device_id={"wide": peer}, device_id_type=MESH,
        ).wait_recv()

    def take(k, c, source):
        for j in range(2):
            slot(k, c, j, source, source).wait_recv()
            use(inb[2 * source + j], code_of(info_ref, source, j))

    take(0, 1, pair)
    keep.wait()
    each(1, 1 + OUT_AHEAD, outward)
    each(0, 1 + ON_AHEAD, onward)
    across(0)

    def arrive(k):
        pl.when(k + BLOCKS_AHEAD <= 15)(lambda: send_block(k + BLOCKS_AHEAD))
        pl.when(k + TILES_AHEAD <= 15)(lambda: send_tiles(k + TILES_AHEAD))
        pl.when(k + OUT_AHEAD <= 15)(lambda: outward(k + OUT_AHEAD))
        dz, dx = step_of(k)
        for c in range(2):
            take(k, c, shifted(me, (dz, dx, c), -1))
        pl.when(k + ON_AHEAD <= 15)(lambda: onward(k + ON_AHEAD))
        across(k)

    each(1, 16, arrive)

    for b in range(NBAT):
        for f in range(FIELDS):
            mine[pl.ds(b * FIELDS + f, 1), :] = jnp.sum(acc[b, f], axis=0, keepdims=True)
    mine[pl.ds(6, 2), :] = jnp.zeros((2, PTS), jnp.float32)
    total = mine[...]
    swaps = []
    for step in range(1, SIDE):
        copy = pltpu.make_async_remote_copy(
            src_ref=mine, dst_ref=parts.at[step - 1], send_sem=part_send.at[step - 1],
            recv_sem=part_recv.at[step - 1], device_id={"narrow": (row + step) % SIDE},
            device_id_type=MESH,
        )
        copy.start()
        swaps.append(copy)
    for copy in sent:
        copy.wait_send()
    for j in range(2):
        slot(0, 1, j, pair, me).wait_send()

    def drain(k):
        plane(k, pair, me).wait_send()
        for c in range(2):
            for j in range(2):
                slot(k, c, j, pair, me).wait_send()

    def finish(k):
        home = home_of(k)
        for side, way in enumerate((1, -1)):
            spread(block, k, home, side, way).wait_send()
        passed(k, home, row, 1).wait_send()
        paired(k, home).wait_send()
        paired(k, shifted(home, (0, 0, 1))).wait_recv()

    each(1, 16, drain)
    each(0, 16, finish)
    for step, copy in enumerate(swaps):
        copy.wait()
        total = total + parts[step]
    dens_ref[...] = total


def dispatch(sel, meta, tiles, ao, occ):
    vmem, smem = pl.BlockSpec(memory_space=pltpu.VMEM), pl.BlockSpec(memory_space=pltpu.SMEM)
    dma = pltpu.SemaphoreType.DMA
    return pl.pallas_call(
        dispatch_kernel,
        out_shape=(
            jax.ShapeDtypeStruct((8, PTS), jnp.float32),
            jax.ShapeDtypeStruct((NWIDE, 8, BLK), jnp.int32),
            jax.ShapeDtypeStruct((NWIDE * SIDE, NOCC, BLK), jnp.bfloat16),
        ),
        in_specs=[smem, vmem, vmem, vmem, vmem],
        out_specs=(vmem, vmem, pl.BlockSpec(memory_space=pltpu.HBM)),
        scratch_shapes=[
            pltpu.VMEM((2 * NWIDE, ROWS, BLK), jnp.bfloat16),
            pltpu.VMEM((2 * NWIDE, ROWS, BLK), jnp.bfloat16),
            pltpu.VMEM((NBAT, FIELDS, 8, PTS), jnp.float32),
            pltpu.VMEM((8, PTS), jnp.float32),
            pltpu.VMEM((SIDE - 1, 8, PTS), jnp.float32),
            pltpu.VMEM((NOCC, BLK), jnp.bfloat16),
            dma((NWIDE, 2)), dma((NWIDE, 2)),
            dma((NWIDE,)), dma((NWIDE,)), dma((SIDE - 1,)), dma((SIDE - 1,)),
            dma, dma((16,)), dma((16,)), dma((16, 2)), dma((16, 2)), dma((16,)), dma((16,)),
            dma((16,)), dma((16,)),
        ],
        compiler_params=pltpu.CompilerParams(
            collective_id=0, has_side_effects=True, vmem_limit_bytes=56 * 2**20
        ),
        cost_estimate=pl.CostEstimate(
            flops=70_000_000_000, bytes_accessed=10_000_000, transcendentals=0
        ),
    )(sel, meta, tiles, ao, occ)


def respond_kernel(
    code_ref, count_ref, dens_ref, weight_ref, first_ref, second_ref, ao_ref, occ_hbm,
    left_hbm, occ, pot, scaled, answer, total, left, head, follow, occ_sem, left_sem,
):
    load_occ = pltpu.make_async_copy(occ_hbm, occ, occ_sem)
    load_occ.start()

    lane = lax.broadcasted_iota(jnp.int32, (1, PTS), 1)
    for b in range(NBAT):
        scale = jnp.where(lane < count_ref[b], weight_ref[pl.ds(b, 1), :], 0.0)
        one, two = first_ref[pl.ds(b, 1), :], second_ref[pl.ds(b, 1), :]
        d = [dens_ref[pl.ds(b * FIELDS + f, 1), :] for f in range(FIELDS)]
        for f in range(FIELDS):
            p, q = d[(f + 1) % 3], d[(f + 2) % 3]
            pot[pl.ds(b * FIELDS + f, 1), :] = scale * (one * d[f] + two * p * q)

    def blocks(i, carry):
        b, f = i // FIELDS, i % FIELDS
        aos = ao_ref[pl.ds(b * KB, KB)].reshape(KB * BLK, PTS)
        scaled[...] = (aos.astype(jnp.float32) * pot[pl.ds(i, 1), :]).astype(jnp.bfloat16)
        part = lax.dot_general(
            scaled[...], aos, (((1,), (1,)), ((), ())), preferred_element_type=jnp.float32
        ).astype(jnp.bfloat16)
        for a in range(KB):
            for c in range(KB):
                answer[b * 25 + a * KB + c, :, pl.ds(pl.multiple_of(f * BLK, BLK), BLK)] = part[
                    a * BLK : (a + 1) * BLK, c * BLK : (c + 1) * BLK
                ]
        return carry

    lax.fori_loop(0, NBAT * FIELDS, blocks, 0)

    def clear(c, carry):
        head[c] = -1
        return carry

    lax.fori_loop(0, 32, clear, 0)

    def link(r, carry):
        code = code_ref[r]
        column = (code // 262144) % 32

        @pl.when((code // 32768) % 2 == 1)
        def _():
            follow[r] = head[column]
            head[column] = r

        return carry

    lax.fori_loop(0, 2 * NWIDE, link, 0)
    load_occ.wait()

    def column_sum(c, carry):
        total[...] = jnp.zeros_like(total)

        def add(r):
            code = code_ref[r]
            block = (r // 2) * 4 + (code // 65536) % 4
            total[...] += jnp.dot(
                occ[block], answer[(code // 512) % 64], preferred_element_type=jnp.float32
            )
            return follow[r]

        lax.while_loop(lambda r: r >= 0, add, head[c])
        slot = c % 2

        @pl.when(c >= 2)
        def _():
            pltpu.make_async_copy(left.at[slot], left_hbm.at[c], left_sem.at[slot]).wait()

        for half in range(2):
            for f in range(FIELDS):
                left[slot, pl.ds(half * HALF + f * 256, 256), :] = total[
                    half * 256 : (half + 1) * 256, f * BLK : (f + 1) * BLK
                ].astype(jnp.bfloat16)
        pltpu.make_async_copy(left.at[slot], left_hbm.at[c], left_sem.at[slot]).start()
        return carry

    lax.fori_loop(0, 32, column_sum, 0)
    for slot in range(2):
        pltpu.make_async_copy(left.at[slot], left_hbm.at[slot], left_sem.at[slot]).wait()


def respond(codes, counts, dens, weights, first, second, ao, occ):
    vmem, smem = pl.BlockSpec(memory_space=pltpu.VMEM), pl.BlockSpec(memory_space=pltpu.SMEM)
    hbm = pl.BlockSpec(memory_space=pltpu.HBM)
    return pl.pallas_call(
        respond_kernel,
        out_shape=jax.ShapeDtypeStruct((32, 2 * HALF, BLK), jnp.bfloat16),
        in_specs=[smem, smem, vmem, vmem, vmem, vmem, vmem, hbm],
        out_specs=hbm,
        scratch_shapes=[
            pltpu.VMEM((128, NOCC, BLK), jnp.bfloat16),
            pltpu.VMEM((8, PTS), jnp.float32),
            pltpu.VMEM((KB * BLK, PTS), jnp.bfloat16),
            pltpu.VMEM((50, BLK, ROWS), jnp.bfloat16),
            pltpu.VMEM((NOCC, ROWS), jnp.float32),
            pltpu.VMEM((2, 2 * HALF, BLK), jnp.bfloat16),
            pltpu.SMEM((32,), jnp.int32),
            pltpu.SMEM((64,), jnp.int32),
            pltpu.SemaphoreType.DMA,
            pltpu.SemaphoreType.DMA((2,)),
        ],
        compiler_params=pltpu.CompilerParams(vmem_limit_bytes=62 * 2**20),
        cost_estimate=pl.CostEstimate(
            flops=30_000_000_000, bytes_accessed=30_000_000, transcendentals=0
        ),
    )(codes, counts, dens, weights, first, second, ao, occ)


def reduce_kernel(
    left_hbm, vir_hbm, out_ref, left, vir, give, got, mid, y_one, x_one, y_sum, x_sum, x_two, y_two,
    left_sem, vir_sem, give_send, give_recv, y_one_send, y_one_recv, x_one_send, x_one_recv,
    x_two_send, x_two_recv, y_two_send, y_two_recv,
):
    me = lax.axis_index("wide")
    row = lax.axis_index("narrow")
    core, chip = me % 2, me // 2
    pair = shifted(me, (0, 0, 1))
    peers = [shifted(me, (z, x, 0)) for z, x in CHIPS]
    barrier = pltpu.get_barrier_semaphore()
    for peer in [pair, *peers]:
        pl.semaphore_signal(barrier, inc=1, device_id={"wide": peer}, device_id_type=MESH)
    for step in range(1, SIDE):
        pl.semaphore_signal(
            barrier, inc=1, device_id={"narrow": (row + step) % SIDE}, device_id_type=MESH
        )

    def load(half, c):
        rows = pl.ds(pl.multiple_of(half * HALF, HALF), HALF)
        return pltpu.make_async_copy(
            left_hbm.at[c, rows],
            left.at[half, :, pl.ds(pl.multiple_of(c * BLK, BLK), BLK)],
            left_sem.at[half, c],
        )

    def load_vir(q):
        return pltpu.make_async_copy(
            vir_hbm.at[:, pl.ds(pl.multiple_of(q * 256, 256), 256)], vir.at[q], vir_sem.at[q]
        )

    def each(last, step):
        def run(k, carry):
            step(k)
            return carry

        lax.fori_loop(0, last, run, 0)

    load_vir(0).start()
    each(32, lambda c: load(1 - core, c).start())
    for q in range(1, SIDE):
        load_vir(q).start()
    each(32, lambda c: load(core, c).start())
    pl.semaphore_wait(barrier, 1 + len(peers) + SIDE - 1)

    def to(axis, peer, src, dst, ssem, rsem):
        return pltpu.make_async_remote_copy(
            src_ref=src, dst_ref=dst, send_sem=ssem, recv_sem=rsem, device_id={axis: peer},
            device_id_type=MESH,
        )

    def product(half, q):
        return jnp.dot(left[half], vir[q], preferred_element_type=jnp.float32).reshape(
            FIELDS, 256, 256
        )

    def hand(q):
        return to("wide", pair, give.at[q], got.at[q], give_send.at[q], give_recv.at[q])

    def other_half(q):
        load_vir(q).wait()
        give[q] = product(1 - core, q).astype(jnp.bfloat16)
        hand(q).start()

    each(32, lambda c: load(1 - core, c).wait())
    each(SIDE, other_half)
    each(32, lambda c: load(core, c).wait())

    def down(q, y):
        return to(
            "narrow", q, mid.at[q, :, :, pl.ds(0, BLK)], y_one.at[y], y_one_send.at[q],
            y_one_recv.at[y],
        )

    def over(q, k, peer):
        rows = pl.ds(pl.multiple_of((peer // 2) * 16, 16), 16)
        return to(
            "wide", peer, mid.at[q, :, rows, pl.ds(BLK, BLK)], x_one.at[k, q],
            x_one_send.at[k, q], x_one_recv.at[k, q],
        )

    def own_half(q):
        own = product(core, q)
        hand(q).wait_recv()
        mid[q] = (own + got[q].astype(jnp.float32)).astype(jnp.bfloat16)
        pl.when(q != row)(lambda: down(q, row).start())
        for k, peer in enumerate(peers):
            over(q, k, peer).start()

    each(SIDE, own_half)
    here = pl.ds(pl.multiple_of(chip * 16, 16), 16)

    total = mid[row, :, :, pl.ds(0, BLK)].astype(jnp.float32)
    for step in range(1, SIDE):
        y = (row + step) % SIDE
        down(y, y).wait_recv()
        total = total + y_one[y].astype(jnp.float32)
    y_sum[...] = total.astype(jnp.bfloat16)

    def scatter(k, peer):
        rows = pl.ds(pl.multiple_of((peer // 2) * 16, 16), 16)
        return to("wide", peer, y_sum.at[:, rows], x_two.at[k], x_two_send.at[k], x_two_recv.at[k])

    for k, peer in enumerate(peers):
        scatter(k, peer).start()

    total = mid[:, :, here, pl.ds(BLK, BLK)].astype(jnp.float32)
    for k, peer in enumerate(peers):
        for q in range(SIDE):
            over(q, k, peer).wait_recv()
        total = total + x_one[k].astype(jnp.float32)
    x_sum[...] = total.astype(jnp.bfloat16)

    def give_row(step):
        y = (row + step) % SIDE
        return to(
            "narrow", y, x_sum.at[y], y_two.at[step - 1], y_two_send.at[step - 1],
            y_two_recv.at[step - 1],
        )

    for step in range(1, SIDE):
        give_row(step).start()

    total = y_sum[:, here].astype(jnp.float32)
    for k, peer in enumerate(peers):
        scatter(k, peer).wait_recv()
        total = total + x_two[k].astype(jnp.float32)
    out_ref[:, :, pl.ds(0, BLK)] = total
    total = x_sum[row].astype(jnp.float32)
    for step in range(1, SIDE):
        give_row(step).wait_recv()
        total = total + y_two[step - 1].astype(jnp.float32)
    out_ref[:, :, pl.ds(BLK, BLK)] = total

    def sent(q):
        hand(q).wait_send()
        pl.when(q != row)(lambda: down(q, row).wait_send())
        for k, peer in enumerate(peers):
            over(q, k, peer).wait_send()

    each(SIDE, sent)
    for k, peer in enumerate(peers):
        scatter(k, peer).wait_send()
    for step in range(1, SIDE):
        give_row(step).wait_send()


def reduced(left, vir):
    hbm = pl.BlockSpec(memory_space=pltpu.HBM)
    dma, bf16 = pltpu.SemaphoreType.DMA, jnp.bfloat16
    chips = len(CHIPS)
    return pl.pallas_call(
        reduce_kernel,
        out_shape=jax.ShapeDtypeStruct((FIELDS, 16, 256), jnp.float32),
        in_specs=[hbm, hbm],
        out_specs=pl.BlockSpec(memory_space=pltpu.VMEM),
        scratch_shapes=[
            pltpu.VMEM((2, HALF, 4096), bf16),
            pltpu.VMEM((SIDE, 4096, 256), bf16),
            pltpu.VMEM((SIDE, FIELDS, 256, 256), bf16),
            pltpu.VMEM((SIDE, FIELDS, 256, 256), bf16),
            pltpu.VMEM((SIDE, FIELDS, 256, 256), bf16),
            pltpu.VMEM((SIDE, FIELDS, 256, BLK), bf16),
            pltpu.VMEM((chips, SIDE, FIELDS, 16, BLK), bf16),
            pltpu.VMEM((FIELDS, 256, BLK), bf16),
            pltpu.VMEM((SIDE, FIELDS, 16, BLK), bf16),
            pltpu.VMEM((chips, FIELDS, 16, BLK), bf16),
            pltpu.VMEM((SIDE - 1, FIELDS, 16, BLK), bf16),
            dma((2, 32)), dma((SIDE,)), dma((SIDE,)), dma((SIDE,)), dma((SIDE,)), dma((SIDE,)),
            dma((chips, SIDE)), dma((chips, SIDE)), dma((chips,)), dma((chips,)),
            dma((SIDE - 1,)), dma((SIDE - 1,)),
        ],
        compiler_params=pltpu.CompilerParams(
            collective_id=1, has_side_effects=True, vmem_limit_bytes=50 * 2**20
        ),
        cost_estimate=pl.CostEstimate(
            flops=30_000_000_000, bytes_accessed=30_000_000, transcendentals=0
        ),
    )(left, vir)


def body(
    dens_tiles,
    tile_dest,
    tile_place,
    tile_rows,
    tile_cols,
    ao_values,
    point_count,
    weights,
    kernel_first,
    kernel_second,
    occ_coef,
    vir_coef,
):
    tile_count = dens_tiles.shape[0]
    targets = tile_dest.reshape(-1)
    routes = jnp.arange(targets.shape[0])
    earlier = (targets[:, None] == targets[None, :]) & (routes[:, None] > routes[None, :])
    position = targets * 2 + jnp.sum(earlier.astype(jnp.int32), axis=1)
    place = tile_place.reshape(-1)
    batch, slot = place // 25, place % 25
    code = (
        (batch * KB + slot // KB) + 16 * (batch * KB + slot % KB) + 256 * batch + 512 * place + 32768
        + 65536 * jnp.repeat(tile_rows, 2) + 262144 * jnp.repeat(tile_cols, 2)
    )
    chosen = position[None, :] == jnp.arange(2 * NWIDE)[:, None]
    sel = jnp.sum(jnp.where(chosen, routes[None, :] // 2, 0), axis=1)
    codes = jnp.sum(jnp.where(chosen, code[None, :], 0), axis=1)
    meta = jnp.broadcast_to(
        jnp.pad(codes.reshape(NWIDE, 1, 2), ((0, 0), (0, 0), (0, BLK - 2))), (NWIDE, 8, BLK)
    )

    ao = ao_values.reshape(NBAT * KB, BLK, PTS)
    dens, info, occ_all = dispatch(
        sel, meta, dens_tiles.reshape(tile_count, ROWS, BLK), ao, occ_coef
    )
    left = respond(
        info[:, 0, :2].reshape(-1), point_count, dens, weights, kernel_first, kernel_second, ao,
        occ_all,
    )
    return reduced(left, vir_coef)


def solution(mesh):
    in_specs = (
        P(("wide", "narrow"), None, None, None),
        P(("wide", "narrow"), None),
        P(("wide", "narrow"), None),
        P(("wide", "narrow")),
        P(("wide", "narrow")),
        P("wide", None, None),
        P("wide"),
        P("wide", None),
        P("wide", None),
        P("wide", None),
        P("wide", None),
        P("narrow", None),
    )
    out_specs = P(None, "wide", "narrow")
    return jax.shard_map(body, mesh=mesh, in_specs=in_specs, out_specs=out_specs, check_vma=False)
```

```python
import jax
import jax.numpy as jnp
from jax import lax
from jax.experimental import pallas as pl
from jax.experimental.pallas import tpu as pltpu
from jax.sharding import PartitionSpec as P

NOCC = 512
NVIR = 1024
BLK = 128
KB = 5
FIELDS = 3
NBAT = 2
PTS = 1280
SIDE = 4
NWIDE = 32
ROWS = FIELDS * BLK
HALF = FIELDS * NOCC // 2
MESH = pl.DeviceIdType.MESH
CHIPS = [(2, 2), (1, 1), (3, 3), (1, 3), (3, 1), (1, 2), (3, 2), (2, 1), (2, 3), (0, 2), (2, 0), (0, 1), (0, 3), (1, 0), (3, 0)]
OUT_AHEAD, TILES_AHEAD, ON_AHEAD = 8, 6, 4
OFFSETS = [(z, x, c) for z, x in CHIPS for c in range(2)] + [(0, 0, 1)]


def shifted(me, offset, sign=1):
    z, x, c = me // 8, (me // 2) % 4, me % 2
    z = (z + sign * offset[0] + 2 * SIDE) % SIDE
    x = (x + sign * offset[1] + 2 * SIDE) % SIDE
    c = (c + offset[2]) % 2
    return z * 8 + x * 2 + c


def number(offset):
    return offset[0] * 8 + offset[1] * 2 + offset[2]


def dispatch_kernel(
    sel_ref, meta_ref, tiles_ref, ao_ref, occ_ref, dens_ref, codes_ref, all_ref,
    info_ref, outb, inb, acc, mine, parts, block,
    send_sem, recv_sem, meta_send, meta_recv, part_send, part_recv,
    own_sem, plane_send, plane_recv, side_send, side_recv, pass_send, pass_recv, pair_send, pair_recv,
):
    me = lax.axis_index("wide")
    row = lax.axis_index("narrow")
    barrier = pltpu.get_barrier_semaphore()
    for offset in OFFSETS:
        pl.semaphore_signal(
            barrier, inc=1, device_id={"wide": shifted(me, offset)}, device_id_type=MESH
        )
    for step in range(1, SIDE):
        pl.semaphore_signal(
            barrier, inc=1, device_id={"narrow": (row + step) % SIDE}, device_id_type=MESH
        )

    turned = occ_ref[pl.ds(pl.multiple_of(row * BLK, BLK), BLK), :].T
    for w in range(NWIDE):
        block[pl.ds((w % 2) * 256 + (w // 2) * 16, 16), :] = turned[w * 16 : (w + 1) * 16]

    def build(i, carry):
        outb[i] = tiles_ref[sel_ref[i]]
        return carry

    lax.fori_loop(0, 2 * NWIDE, build, 0)
    acc[...] = jnp.zeros_like(acc)
    pl.semaphore_wait(barrier, len(OFFSETS) + SIDE - 1)

    sent = []

    def send(src, dst, ssem, rsem, peer):
        copy = pltpu.make_async_remote_copy(
            src_ref=src, dst_ref=dst, send_sem=ssem, recv_sem=rsem,
            device_id={"wide": peer}, device_id_type=MESH,
        )
        copy.start()
        sent.append(copy)

    for offset in OFFSETS:
        peer, k = shifted(me, offset), number(offset)
        send(meta_ref.at[peer], info_ref.at[me], meta_send.at[k], meta_recv.at[k], peer)
    info_ref[me] = meta_ref[me]

    def step_of(k):
        dz = sum(jnp.where(k == n + 1, z, 0) for n, (z, _) in enumerate(CHIPS))
        dx = sum(jnp.where(k == n + 1, x, 0) for n, (_, x) in enumerate(CHIPS))
        return dz, dx

    core = me % 2

    def turn(k):
        d, e = k % 4, k // 4
        return e + core * (d - e), d + core * (e - d)

    def home_of(k):
        return shifted(me, (*turn(k), 0), -1)

    def slot(k, c, j, peer, source):
        return pltpu.make_async_remote_copy(
            src_ref=outb.at[2 * peer + j], dst_ref=inb.at[2 * source + j],
            send_sem=send_sem.at[2 * k + c, j], recv_sem=recv_sem.at[2 * k + c, j],
            device_id={"wide": peer}, device_id_type=MESH,
        )

    def send_tiles(k):
        dz, dx = step_of(k)
        for c in range(2):
            for j in range(2):
                slot(k, c, j, shifted(me, (dz, dx, c)), me).start()

    def place(home, y):
        return all_ref.at[home * SIDE + (y + 2 * SIDE) % SIDE]

    def plane(k, peer, home, src=block):
        return pltpu.make_async_remote_copy(
            src_ref=src, dst_ref=place(home, row), send_sem=plane_send.at[k],
            recv_sem=plane_recv.at[k], device_id={"wide": peer}, device_id_type=MESH,
        )

    def send_block(k):
        plane(k, shifted(me, (*turn(k), 0)), me).start()

    def spread(src, k, home, side, way):
        return pltpu.make_async_remote_copy(
            src_ref=src, dst_ref=place(home, row), send_sem=side_send.at[k, side],
            recv_sem=side_recv.at[k, side], device_id={"narrow": (row + way + SIDE) % SIDE},
            device_id_type=MESH,
        )

    def passed(k, home, y, way):
        return pltpu.make_async_remote_copy(
            src_ref=place(home, y), dst_ref=place(home, y), send_sem=pass_send.at[k],
            recv_sem=pass_recv.at[k], device_id={"narrow": (row + way + SIDE) % SIDE},
            device_id_type=MESH,
        )

    def paired(k, home):
        four = all_ref.at[pl.ds(home * SIDE, SIDE)]
        return pltpu.make_async_remote_copy(
            src_ref=four, dst_ref=four, send_sem=pair_send.at[k], recv_sem=pair_recv.at[k],
            device_id={"wide": shifted(me, (0, 0, 1))}, device_id_type=MESH,
        )

    def outward(k):
        home = home_of(k)
        plane(k, home, home).wait_recv()
        for side, way in enumerate((1, -1)):
            spread(place(home, row), k, home, side, way).start()

    def forward(k):
        home = home_of(k)
        for e in range(1, SIDE):
            plane(
                4 * e + k, shifted(me, (*turn(4 * e), 0)), home, place(home, row)
            ).start()

    def onward(k):
        home = home_of(k)
        for side, way in enumerate((1, -1)):
            pltpu.make_async_remote_copy(
                src_ref=block, dst_ref=place(home, row - way), send_sem=side_send.at[k, side],
                recv_sem=side_recv.at[k, side], device_id={"narrow": (row - way + SIDE) % SIDE},
                device_id_type=MESH,
            ).wait_recv()
        way = 1 - 2 * (k % 2)
        passed(k, home, row - way, way).start()

    def across(k):
        home = home_of(k)
        passed(k, home, row + 2, 1).wait_recv()
        paired(k, home).start()

    def each(first, last, step):
        def run(k, carry):
            step(k)
            return carry

        lax.fori_loop(first, last, run, 0)

    keep = pltpu.make_async_copy(block, place(me, row), own_sem)
    keep.start()
    for side, way in enumerate((1, -1)):
        spread(block, 0, me, side, way).start()
    pair = shifted(me, (0, 0, 1))
    for k in (1, 2, 3, 4, 8, 12):
        send_block(k)
    for j in range(2):
        slot(0, 1, j, pair, me).start()
    send_tiles(1)

    def relay(k):
        outward(k)
        forward(k)

    each(1, SIDE, relay)
    each(2, 1 + TILES_AHEAD, send_tiles)

    def use(tile, code):
        first, second = code % 16, (code // 16) % 16
        batch, valid = (code // 256) % 2, (code // 32768) % 2
        lives = [jnp.logical_and(valid == 1, batch == b) for b in range(NBAT)]
        for q in range(PTS // 256):
            cols = pl.ds(q * 256, 256)
            mixed = jnp.dot(tile, ao_ref[second, :, cols], preferred_element_type=jnp.float32)
            left = ao_ref[first, :, cols].astype(jnp.float32)
            part = jnp.sum(
                mixed.reshape(FIELDS, BLK // 8, 8, 256) * left.reshape(1, BLK // 8, 8, 256), axis=1
            )
            for b in range(NBAT):
                acc[b, :, :, cols] += jnp.where(lives[b], part, 0.0)

    def code_of(ref, source, j):
        return ref[source, 0:1, j : j + 1][0, 0]

    for j in range(2):
        code = code_of(meta_ref, me, j)
        codes_ref[2 * me + j] = code
        use(outb[2 * me + j], code)

    for offset in OFFSETS:
        peer, k = shifted(me, offset), number(offset)
        pltpu.make_async_remote_copy(
            src_ref=meta_ref.at[0], dst_ref=info_ref.at[0], send_sem=meta_send.at[k],
            recv_sem=meta_recv.at[k], device_id={"wide": peer}, device_id_type=MESH,
        ).wait_recv()

    def take(k, c, source):
        for j in range(2):
            slot(k, c, j, source, source).wait_recv()
            code = code_of(info_ref, source, j)
            codes_ref[2 * source + j] = code
            use(inb[2 * source + j], code)

    take(0, 1, pair)
    keep.wait()
    each(SIDE, 1 + OUT_AHEAD, outward)
    each(0, 1 + ON_AHEAD, onward)
    across(0)

    def arrive(k):
        pl.when(k + TILES_AHEAD <= 15)(lambda: send_tiles(k + TILES_AHEAD))
        pl.when(k + OUT_AHEAD <= 15)(lambda: outward(k + OUT_AHEAD))
        dz, dx = step_of(k)
        for c in range(2):
            take(k, c, shifted(me, (dz, dx, c), -1))
        pl.when(k + ON_AHEAD <= 15)(lambda: onward(k + ON_AHEAD))
        across(k)

    each(1, 16, arrive)

    for b in range(NBAT):
        for f in range(FIELDS):
            mine[pl.ds(b * FIELDS + f, 1), :] = jnp.sum(acc[b, f], axis=0, keepdims=True)
    mine[pl.ds(6, 2), :] = jnp.zeros((2, PTS), jnp.float32)
    total = mine[...]
    swaps = []
    for step in range(1, SIDE):
        copy = pltpu.make_async_remote_copy(
            src_ref=mine, dst_ref=parts.at[step - 1], send_sem=part_send.at[step - 1],
            recv_sem=part_recv.at[step - 1], device_id={"narrow": (row + step) % SIDE},
            device_id_type=MESH,
        )
        copy.start()
        swaps.append(copy)
    for copy in sent:
        copy.wait_send()
    for j in range(2):
        slot(0, 1, j, pair, me).wait_send()

    def drain(k):
        plane(k, pair, me).wait_send()
        for c in range(2):
            for j in range(2):
                slot(k, c, j, pair, me).wait_send()

    def finish(k):
        home = home_of(k)
        for side, way in enumerate((1, -1)):
            spread(block, k, home, side, way).wait_send()
        passed(k, home, row, 1).wait_send()
        paired(k, home).wait_send()
        dz, dx = turn(k)
        paired(k, shifted(me, (dx, dz, 1), -1)).wait_recv()

    each(1, 16, drain)
    each(0, 16, finish)
    for step, copy in enumerate(swaps):
        copy.wait()
        total = total + parts[step]
    dens_ref[...] = total


def dispatch(sel, meta, tiles, ao, occ):
    vmem, smem = pl.BlockSpec(memory_space=pltpu.VMEM), pl.BlockSpec(memory_space=pltpu.SMEM)
    dma = pltpu.SemaphoreType.DMA
    return pl.pallas_call(
        dispatch_kernel,
        out_shape=(
            jax.ShapeDtypeStruct((8, PTS), jnp.float32),
            jax.ShapeDtypeStruct((2 * NWIDE,), jnp.int32),
            jax.ShapeDtypeStruct((NWIDE * SIDE, NOCC, BLK), jnp.bfloat16),
        ),
        in_specs=[smem, vmem, vmem, vmem, vmem],
        out_specs=(vmem, smem, pl.BlockSpec(memory_space=pltpu.HBM)),
        scratch_shapes=[
            pltpu.VMEM((NWIDE, 8, BLK), jnp.int32),
            pltpu.VMEM((2 * NWIDE, ROWS, BLK), jnp.bfloat16),
            pltpu.VMEM((2 * NWIDE, ROWS, BLK), jnp.bfloat16),
            pltpu.VMEM((NBAT, FIELDS, 8, PTS), jnp.float32),
            pltpu.VMEM((8, PTS), jnp.float32),
            pltpu.VMEM((SIDE - 1, 8, PTS), jnp.float32),
            pltpu.VMEM((NOCC, BLK), jnp.bfloat16),
            dma((NWIDE, 2)), dma((NWIDE, 2)),
            dma((NWIDE,)), dma((NWIDE,)), dma((SIDE - 1,)), dma((SIDE - 1,)),
            dma, dma((16,)), dma((16,)), dma((16, 2)), dma((16, 2)), dma((16,)), dma((16,)),
            dma((16,)), dma((16,)),
        ],
        compiler_params=pltpu.CompilerParams(
            collective_id=0, has_side_effects=True, vmem_limit_bytes=56 * 2**20
        ),
        cost_estimate=pl.CostEstimate(
            flops=70_000_000_000, bytes_accessed=10_000_000, transcendentals=0
        ),
    )(sel, meta, tiles, ao, occ)


def respond_kernel(
    code_ref, count_ref, dens_ref, weight_ref, first_ref, second_ref, ao_ref, occ_hbm,
    left_hbm, occ, pot, scaled, answer, total, left, head, follow, occ_sem, left_sem,
):
    load_occ = pltpu.make_async_copy(occ_hbm, occ, occ_sem)
    load_occ.start()

    lane = lax.broadcasted_iota(jnp.int32, (1, PTS), 1)
    for b in range(NBAT):
        scale = jnp.where(lane < count_ref[b], weight_ref[pl.ds(b, 1), :], 0.0)
        one, two = first_ref[pl.ds(b, 1), :], second_ref[pl.ds(b, 1), :]
        d = [dens_ref[pl.ds(b * FIELDS + f, 1), :] for f in range(FIELDS)]
        for f in range(FIELDS):
            p, q = d[(f + 1) % 3], d[(f + 2) % 3]
            pot[pl.ds(b * FIELDS + f, 1), :] = scale * (one * d[f] + two * p * q)

    def blocks(i, carry):
        b, f = i // FIELDS, i % FIELDS
        aos = ao_ref[pl.ds(b * KB, KB)].reshape(KB * BLK, PTS)
        scaled[...] = (aos.astype(jnp.float32) * pot[pl.ds(i, 1), :]).astype(jnp.bfloat16)
        part = lax.dot_general(
            scaled[...], aos, (((1,), (1,)), ((), ())), preferred_element_type=jnp.float32
        ).astype(jnp.bfloat16)
        for a in range(KB):
            for c in range(KB):
                answer[b * 25 + a * KB + c, :, pl.ds(pl.multiple_of(f * BLK, BLK), BLK)] = part[
                    a * BLK : (a + 1) * BLK, c * BLK : (c + 1) * BLK
                ]
        return carry

    lax.fori_loop(0, NBAT * FIELDS, blocks, 0)

    def clear(c, carry):
        head[c] = -1
        follow[2 * c] = -1
        follow[2 * c + 1] = -1
        return carry

    lax.fori_loop(0, 32, clear, 0)

    def link(r, carry):
        code = code_ref[r]
        column = (code // 262144) % 32

        @pl.when((code // 32768) % 2 == 1)
        def _():
            follow[r] = head[column]
            head[column] = r

        return carry

    lax.fori_loop(0, 2 * NWIDE, link, 0)
    load_occ.wait()

    def column_sum(c, carry):
        def term(r):
            code = code_ref[r]
            return occ[(r // 2) * 4 + (code // 65536) % 4], answer[(code // 512) % 64]

        def two(r):
            nxt = follow[r]
            other = jnp.where(nxt >= 0, nxt, r)
            (left_a, right_a), (left_b, right_b) = term(r), term(other)
            right_b = jnp.where(nxt >= 0, right_b, jnp.zeros_like(right_b))
            return jnp.dot(
                jnp.concatenate([left_a, left_b], axis=1),
                jnp.concatenate([right_a, right_b], axis=0), preferred_element_type=jnp.float32,
            )

        def after(r):
            nxt = follow[jnp.maximum(r, 0)]
            last = jnp.logical_or(r < 0, nxt < 0)
            return jnp.where(last, -1, follow[jnp.maximum(nxt, 0)])

        def add(r):
            total[...] += two(r)
            return after(r)

        first = head[c]

        @pl.when(first < 0)
        def _():
            total[...] = jnp.zeros_like(total)

        @pl.when(first >= 0)
        def _():
            total[...] = two(first)

        lax.while_loop(lambda r: r >= 0, add, after(first))
        slot = c % 2

        @pl.when(c >= 2)
        def _():
            pltpu.make_async_copy(left.at[slot], left_hbm.at[c], left_sem.at[slot]).wait()

        for half in range(2):
            for f in range(FIELDS):
                left[slot, pl.ds(half * HALF + f * 256, 256), :] = total[
                    half * 256 : (half + 1) * 256, f * BLK : (f + 1) * BLK
                ].astype(jnp.bfloat16)
        pltpu.make_async_copy(left.at[slot], left_hbm.at[c], left_sem.at[slot]).start()
        return carry

    lax.fori_loop(0, 32, column_sum, 0)
    for slot in range(2):
        pltpu.make_async_copy(left.at[slot], left_hbm.at[slot], left_sem.at[slot]).wait()


def respond(codes, counts, dens, weights, first, second, ao, occ):
    vmem, smem = pl.BlockSpec(memory_space=pltpu.VMEM), pl.BlockSpec(memory_space=pltpu.SMEM)
    hbm = pl.BlockSpec(memory_space=pltpu.HBM)
    return pl.pallas_call(
        respond_kernel,
        out_shape=jax.ShapeDtypeStruct((32, 2 * HALF, BLK), jnp.bfloat16),
        in_specs=[smem, smem, vmem, vmem, vmem, vmem, vmem, hbm],
        out_specs=hbm,
        scratch_shapes=[
            pltpu.VMEM((128, NOCC, BLK), jnp.bfloat16),
            pltpu.VMEM((8, PTS), jnp.float32),
            pltpu.VMEM((KB * BLK, PTS), jnp.bfloat16),
            pltpu.VMEM((50, BLK, ROWS), jnp.bfloat16),
            pltpu.VMEM((NOCC, ROWS), jnp.float32),
            pltpu.VMEM((2, 2 * HALF, BLK), jnp.bfloat16),
            pltpu.SMEM((32,), jnp.int32),
            pltpu.SMEM((64,), jnp.int32),
            pltpu.SemaphoreType.DMA,
            pltpu.SemaphoreType.DMA((2,)),
        ],
        compiler_params=pltpu.CompilerParams(vmem_limit_bytes=62 * 2**20),
        cost_estimate=pl.CostEstimate(
            flops=30_000_000_000, bytes_accessed=30_000_000, transcendentals=0
        ),
    )(codes, counts, dens, weights, first, second, ao, occ)


def reduce_kernel(
    left_hbm, vir_hbm, out_ref, left, vir, give, got, mid, y_one, x_one, y_sum, x_sum, x_two, y_two,
    left_sem, vir_sem, give_send, give_recv, y_one_send, y_one_recv, x_one_send, x_one_recv,
    x_two_send, x_two_recv, y_two_send, y_two_recv,
):
    me = lax.axis_index("wide")
    row = lax.axis_index("narrow")
    core, chip = me % 2, me // 2
    pair = shifted(me, (0, 0, 1))
    peers = [shifted(me, (z, x, 0)) for z, x in CHIPS]
    barrier = pltpu.get_barrier_semaphore()
    for peer in [pair, *peers]:
        pl.semaphore_signal(barrier, inc=1, device_id={"wide": peer}, device_id_type=MESH)
    for step in range(1, SIDE):
        pl.semaphore_signal(
            barrier, inc=1, device_id={"narrow": (row + step) % SIDE}, device_id_type=MESH
        )

    def load(half, c):
        rows = pl.ds(pl.multiple_of(half * HALF, HALF), HALF)
        return pltpu.make_async_copy(
            left_hbm.at[c, rows],
            left.at[half, :, pl.ds(pl.multiple_of(c * BLK, BLK), BLK)],
            left_sem.at[half, c],
        )

    def load_vir(q):
        return pltpu.make_async_copy(
            vir_hbm.at[:, pl.ds(pl.multiple_of(q * 256, 256), 256)], vir.at[q], vir_sem.at[q]
        )

    def each(last, step):
        def run(k, carry):
            step(k)
            return carry

        lax.fori_loop(0, last, run, 0)

    load_vir(0).start()
    each(32, lambda c: load(1 - core, c).start())
    for q in range(1, SIDE):
        load_vir(q).start()
    each(32, lambda c: load(core, c).start())
    pl.semaphore_wait(barrier, 1 + len(peers) + SIDE - 1)

    def to(axis, peer, src, dst, ssem, rsem):
        return pltpu.make_async_remote_copy(
            src_ref=src, dst_ref=dst, send_sem=ssem, recv_sem=rsem, device_id={axis: peer},
            device_id_type=MESH,
        )

    def product(half, q):
        return jnp.dot(left[half], vir[q], preferred_element_type=jnp.float32).reshape(
            FIELDS, 256, 256
        )

    def hand(q):
        return to("wide", pair, give.at[q], got.at[q], give_send.at[q], give_recv.at[q])

    def other_half(q):
        load_vir(q).wait()
        give[q] = product(1 - core, q).astype(jnp.bfloat16)
        hand(q).start()

    each(32, lambda c: load(1 - core, c).wait())
    each(SIDE, other_half)
    each(32, lambda c: load(core, c).wait())

    def down(q, y):
        return to(
            "narrow", q, mid.at[q, :, :, pl.ds(0, BLK)], y_one.at[y], y_one_send.at[q],
            y_one_recv.at[y],
        )

    def over(q, k, peer):
        rows = pl.ds(pl.multiple_of((peer // 2) * 16, 16), 16)
        return to(
            "wide", peer, mid.at[q, :, rows, pl.ds(BLK, BLK)], x_one.at[k, q],
            x_one_send.at[k, q], x_one_recv.at[k, q],
        )

    def own_half(q):
        own = product(core, q)
        hand(q).wait_recv()
        mid[q] = (own + got[q].astype(jnp.float32)).astype(jnp.bfloat16)
        pl.when(q != row)(lambda: down(q, row).start())
        for k, peer in enumerate(peers):
            over(q, k, peer).start()

    each(SIDE, own_half)
    here = pl.ds(pl.multiple_of(chip * 16, 16), 16)

    total = mid[row, :, :, pl.ds(0, BLK)].astype(jnp.float32)
    for step in range(1, SIDE):
        y = (row + step) % SIDE
        down(y, y).wait_recv()
        total = total + y_one[y].astype(jnp.float32)
    y_sum[...] = total.astype(jnp.bfloat16)

    def scatter(k, peer):
        rows = pl.ds(pl.multiple_of((peer // 2) * 16, 16), 16)
        return to("wide", peer, y_sum.at[:, rows], x_two.at[k], x_two_send.at[k], x_two_recv.at[k])

    for k, peer in enumerate(peers):
        scatter(k, peer).start()

    total = mid[:, :, here, pl.ds(BLK, BLK)].astype(jnp.float32)
    for k, peer in enumerate(peers):
        for q in range(SIDE):
            over(q, k, peer).wait_recv()
        total = total + x_one[k].astype(jnp.float32)
    x_sum[...] = total.astype(jnp.bfloat16)

    def give_row(step):
        y = (row + step) % SIDE
        return to(
            "narrow", y, x_sum.at[y], y_two.at[step - 1], y_two_send.at[step - 1],
            y_two_recv.at[step - 1],
        )

    for step in range(1, SIDE):
        give_row(step).start()

    total = y_sum[:, here].astype(jnp.float32)
    for k, peer in enumerate(peers):
        scatter(k, peer).wait_recv()
        total = total + x_two[k].astype(jnp.float32)
    out_ref[:, :, pl.ds(0, BLK)] = total
    total = x_sum[row].astype(jnp.float32)
    for step in range(1, SIDE):
        give_row(step).wait_recv()
        total = total + y_two[step - 1].astype(jnp.float32)
    out_ref[:, :, pl.ds(BLK, BLK)] = total

    def sent(q):
        hand(q).wait_send()
        pl.when(q != row)(lambda: down(q, row).wait_send())
        for k, peer in enumerate(peers):
            over(q, k, peer).wait_send()

    each(SIDE, sent)
    for k, peer in enumerate(peers):
        scatter(k, peer).wait_send()
    for step in range(1, SIDE):
        give_row(step).wait_send()


def reduced(left, vir):
    hbm = pl.BlockSpec(memory_space=pltpu.HBM)
    dma, bf16 = pltpu.SemaphoreType.DMA, jnp.bfloat16
    chips = len(CHIPS)
    return pl.pallas_call(
        reduce_kernel,
        out_shape=jax.ShapeDtypeStruct((FIELDS, 16, 256), jnp.float32),
        in_specs=[hbm, hbm],
        out_specs=pl.BlockSpec(memory_space=pltpu.VMEM),
        scratch_shapes=[
            pltpu.VMEM((2, HALF, 4096), bf16),
            pltpu.VMEM((SIDE, 4096, 256), bf16),
            pltpu.VMEM((SIDE, FIELDS, 256, 256), bf16),
            pltpu.VMEM((SIDE, FIELDS, 256, 256), bf16),
            pltpu.VMEM((SIDE, FIELDS, 256, 256), bf16),
            pltpu.VMEM((SIDE, FIELDS, 256, BLK), bf16),
            pltpu.VMEM((chips, SIDE, FIELDS, 16, BLK), bf16),
            pltpu.VMEM((FIELDS, 256, BLK), bf16),
            pltpu.VMEM((SIDE, FIELDS, 16, BLK), bf16),
            pltpu.VMEM((chips, FIELDS, 16, BLK), bf16),
            pltpu.VMEM((SIDE - 1, FIELDS, 16, BLK), bf16),
            dma((2, 32)), dma((SIDE,)), dma((SIDE,)), dma((SIDE,)), dma((SIDE,)), dma((SIDE,)),
            dma((chips, SIDE)), dma((chips, SIDE)), dma((chips,)), dma((chips,)),
            dma((SIDE - 1,)), dma((SIDE - 1,)),
        ],
        compiler_params=pltpu.CompilerParams(
            collective_id=1, has_side_effects=True, vmem_limit_bytes=50 * 2**20
        ),
        cost_estimate=pl.CostEstimate(
            flops=30_000_000_000, bytes_accessed=30_000_000, transcendentals=0
        ),
    )(left, vir)


def body(
    dens_tiles,
    tile_dest,
    tile_place,
    tile_rows,
    tile_cols,
    ao_values,
    point_count,
    weights,
    kernel_first,
    kernel_second,
    occ_coef,
    vir_coef,
):
    tile_count = dens_tiles.shape[0]
    targets = tile_dest.reshape(-1)
    routes = jnp.arange(targets.shape[0])
    earlier = (targets[:, None] == targets[None, :]) & (routes[:, None] > routes[None, :])
    position = targets * 2 + jnp.sum(earlier.astype(jnp.int32), axis=1)
    place = tile_place.reshape(-1)
    batch, slot = place // 25, place % 25
    code = (
        (batch * KB + slot // KB) + 16 * (batch * KB + slot % KB) + 256 * batch + 512 * place + 32768
        + 65536 * jnp.repeat(tile_rows, 2) + 262144 * jnp.repeat(tile_cols, 2)
    )
    chosen = position[None, :] == jnp.arange(2 * NWIDE)[:, None]
    sel = jnp.sum(jnp.where(chosen, routes[None, :] // 2, 0), axis=1)
    sent = jnp.sum(jnp.where(chosen, code[None, :], 0), axis=1)
    meta = jnp.broadcast_to(
        jnp.pad(sent.reshape(NWIDE, 1, 2), ((0, 0), (0, 0), (0, BLK - 2))), (NWIDE, 8, BLK)
    )

    ao = ao_values.reshape(NBAT * KB, BLK, PTS)
    dens, codes, occ_all = dispatch(
        sel, meta, dens_tiles.reshape(tile_count, ROWS, BLK), ao, occ_coef
    )
    left = respond(
        codes, point_count, dens, weights, kernel_first, kernel_second, ao,
        occ_all,
    )
    return reduced(left, vir_coef)


def solution(mesh):
    in_specs = (
        P(("wide", "narrow"), None, None, None),
        P(("wide", "narrow"), None),
        P(("wide", "narrow"), None),
        P(("wide", "narrow")),
        P(("wide", "narrow")),
        P("wide", None, None),
        P("wide"),
        P("wide", None),
        P("wide", None),
        P("wide", None),
        P("wide", None),
        P("narrow", None),
    )
    out_specs = P(None, "wide", "narrow")
    return jax.shard_map(body, mesh=mesh, in_specs=in_specs, out_specs=out_specs, check_vma=False)
```

```python
import jax
import jax.numpy as jnp
from jax import lax
from jax.experimental import pallas as pl
from jax.experimental.pallas import tpu as pltpu
from jax.sharding import PartitionSpec as P

NOCC = 512
NVIR = 1024
BLK = 128
KB = 5
FIELDS = 3
NBAT = 2
PTS = 1280
SIDE = 4
NWIDE = 32
TILES = 16
ROWS = FIELDS * BLK
HALF = FIELDS * NOCC // 2
MESH = pl.DeviceIdType.MESH
CHIPS = [(2, 2), (1, 1), (3, 3), (1, 3), (3, 1), (1, 2), (3, 2), (2, 1), (2, 3), (0, 2), (2, 0), (0, 1), (0, 3), (1, 0), (3, 0)]
OUT_AHEAD, TILES_AHEAD, ON_AHEAD = 8, 6, 4
OFFSETS = [(z, x, c) for z, x in CHIPS for c in range(2)] + [(0, 0, 1)]


def shifted(me, offset, sign=1):
    z, x, c = me // 8, (me // 2) % 4, me % 2
    z = (z + sign * offset[0] + 2 * SIDE) % SIDE
    x = (x + sign * offset[1] + 2 * SIDE) % SIDE
    c = (c + offset[2]) % 2
    return z * 8 + x * 2 + c


def dispatch_kernel(
    dest_ref, place_ref, rows_ref, cols_ref, tiles_hbm, ao_hbm, occ_hbm, dens_ref, codes_ref, all_ref,
    tiles_ref, ao_ref, occ_ref, load_sem, meta_ref, info_ref, outb, inb, acc, mine, parts, block,
    send_sem, recv_sem, meta_send, meta_recv, part_send, part_recv,
    own_sem, plane_send, plane_recv, side_send, side_recv, pass_send, pass_recv, pair_send, pair_recv,
):
    me = lax.axis_index("wide")
    row = lax.axis_index("narrow")
    quarter = pl.ds(pl.multiple_of(row * BLK, BLK), BLK)
    load_occ = pltpu.make_async_copy(occ_hbm.at[quarter], occ_ref, load_sem.at[0])
    load_tiles = pltpu.make_async_copy(tiles_hbm, tiles_ref, load_sem.at[1])
    load_ao = pltpu.make_async_copy(ao_hbm, ao_ref, load_sem.at[2])
    load_occ.start()
    load_tiles.start()
    load_ao.start()
    barrier = pltpu.get_barrier_semaphore()
    for offset in OFFSETS:
        pl.semaphore_signal(
            barrier, inc=1, device_id={"wide": shifted(me, offset)}, device_id_type=MESH
        )
    for step in range(1, SIDE):
        pl.semaphore_signal(
            barrier, inc=1, device_id={"narrow": (row + step) % SIDE}, device_id_type=MESH
        )

    load_occ.wait()
    turned = occ_ref[...].T
    for w in range(NWIDE):
        block[pl.ds((w % 2) * 256 + (w // 2) * 16, 16), :] = turned[w * 16 : (w + 1) * 16]

    acc[...] = jnp.zeros_like(acc)
    pl.semaphore_wait(barrier, len(OFFSETS) + SIDE - 1)

    def step_of(k):
        dz = sum(jnp.where(k == n + 1, z, 0) for n, (z, _) in enumerate(CHIPS))
        dx = sum(jnp.where(k == n + 1, x, 0) for n, (_, x) in enumerate(CHIPS))
        return dz, dx

    core = me % 2

    def turn(k):
        d, e = k % 4, k // 4
        return e + core * (d - e), d + core * (e - d)

    def home_of(k):
        return shifted(me, (*turn(k), 0), -1)

    def slot(k, c, j, peer, source):
        return pltpu.make_async_remote_copy(
            src_ref=outb.at[2 * peer + j], dst_ref=inb.at[2 * source + j],
            send_sem=send_sem.at[2 * k + c, j], recv_sem=recv_sem.at[2 * k + c, j],
            device_id={"wide": peer}, device_id_type=MESH,
        )

    def info(k, peer, source):
        return pltpu.make_async_remote_copy(
            src_ref=meta_ref.at[peer], dst_ref=info_ref.at[source], send_sem=meta_send.at[k],
            recv_sem=meta_recv.at[k], device_id={"wide": peer}, device_id_type=MESH,
        )

    def send_tiles(k):
        dz, dx = step_of(k)
        for c in range(2):
            info(2 * k + c, shifted(me, (dz, dx, c)), me).start()
            for j in range(2):
                slot(k, c, j, shifted(me, (dz, dx, c)), me).start()

    def place(home, y):
        return all_ref.at[home * SIDE + (y + 2 * SIDE) % SIDE]

    def plane(k, peer, home, src=block):
        return pltpu.make_async_remote_copy(
            src_ref=src, dst_ref=place(home, row), send_sem=plane_send.at[k],
            recv_sem=plane_recv.at[k], device_id={"wide": peer}, device_id_type=MESH,
        )

    def send_block(k):
        plane(k, shifted(me, (*turn(k), 0)), me).start()

    def spread(src, k, home, side, way):
        return pltpu.make_async_remote_copy(
            src_ref=src, dst_ref=place(home, row), send_sem=side_send.at[k, side],
            recv_sem=side_recv.at[k, side], device_id={"narrow": (row + way + SIDE) % SIDE},
            device_id_type=MESH,
        )

    def passed(k, home, y, way):
        return pltpu.make_async_remote_copy(
            src_ref=place(home, y), dst_ref=place(home, y), send_sem=pass_send.at[k],
            recv_sem=pass_recv.at[k], device_id={"narrow": (row + way + SIDE) % SIDE},
            device_id_type=MESH,
        )

    def paired(k, home):
        four = all_ref.at[pl.ds(home * SIDE, SIDE)]
        return pltpu.make_async_remote_copy(
            src_ref=four, dst_ref=four, send_sem=pair_send.at[k], recv_sem=pair_recv.at[k],
            device_id={"wide": shifted(me, (0, 0, 1))}, device_id_type=MESH,
        )

    def outward(k):
        home = home_of(k)
        plane(k, home, home).wait_recv()
        for side, way in enumerate((1, -1)):
            spread(place(home, row), k, home, side, way).start()

    def forward(k):
        home = home_of(k)
        for e in range(1, SIDE):
            plane(
                4 * e + k, shifted(me, (*turn(4 * e), 0)), home, place(home, row)
            ).start()

    def onward(k):
        home = home_of(k)
        for side, way in enumerate((1, -1)):
            pltpu.make_async_remote_copy(
                src_ref=block, dst_ref=place(home, row - way), send_sem=side_send.at[k, side],
                recv_sem=side_recv.at[k, side], device_id={"narrow": (row - way + SIDE) % SIDE},
                device_id_type=MESH,
            ).wait_recv()
        way = 1 - 2 * (k % 2)
        passed(k, home, row - way, way).start()

    def across(k):
        home = home_of(k)
        passed(k, home, row + 2, 1).wait_recv()
        paired(k, home).start()

    def each(first, last, step):
        def run(k, carry):
            step(k)
            return carry

        lax.fori_loop(first, last, run, 0)

    keep = pltpu.make_async_copy(block, place(me, row), own_sem)
    keep.start()
    for side, way in enumerate((1, -1)):
        spread(block, 0, me, side, way).start()
    pair = shifted(me, (0, 0, 1))
    for k in (1, 2, 3, 4, 8, 12):
        send_block(k)
    load_tiles.wait()
    lane = lax.broadcasted_iota(jnp.int32, (8, BLK), 1)

    def route(peer):
        found = [-1, -1]
        for r in range(2 * TILES):
            hit = dest_ref[r % 2, r // 2] == peer
            found = [
                jnp.where(jnp.logical_and(hit, found[0] < 0), r, found[0]),
                jnp.where(jnp.logical_and(hit, found[0] >= 0), r, found[1]),
            ]
        codes = []
        for j in range(2):
            r = jnp.maximum(found[j], 0)
            t = r // 2
            spot = place_ref[r % 2, t]
            batch, block_pair = spot // 25, spot % 25
            code = (
                (batch * KB + block_pair // KB) + 16 * (batch * KB + block_pair % KB) + 256 * batch
                + 512 * spot + 32768 + 65536 * rows_ref[t] + 262144 * cols_ref[t]
            )
            codes.append(jnp.where(found[j] >= 0, code, 0))
            outb[2 * peer + j] = tiles_ref[t]
        meta_ref[peer] = jnp.where(lane == 0, codes[0], jnp.where(lane == 1, codes[1], 0))

    def route_chip(k):
        dz, dx = step_of(k)
        for c in range(2):
            route(shifted(me, (dz, dx, c)))

    def advance(k):
        pl.when(k < 15)(lambda: route_chip(k + 1))
        send_tiles(k)

    route(pair)
    route(me)
    route_chip(1)
    info(1, pair, me).start()
    for j in range(2):
        slot(0, 1, j, pair, me).start()
    advance(1)

    def relay(k):
        outward(k)
        forward(k)

    each(1, SIDE, relay)
    each(2, 1 + TILES_AHEAD, advance)

    def use(tile, code):
        first, second = code % 16, (code // 16) % 16
        batch, valid = (code // 256) % 2, (code // 32768) % 2
        lives = [jnp.logical_and(valid == 1, batch == b) for b in range(NBAT)]
        for q in range(PTS // 256):
            cols = pl.ds(q * 256, 256)
            mixed = jnp.dot(tile, ao_ref[second, :, cols], preferred_element_type=jnp.float32)
            left = ao_ref[first, :, cols].astype(jnp.float32)
            part = jnp.sum(
                mixed.reshape(FIELDS, BLK // 8, 8, 256) * left.reshape(1, BLK // 8, 8, 256), axis=1
            )
            for b in range(NBAT):
                acc[b, :, :, cols] += jnp.where(lives[b], part, 0.0)

    def code_of(ref, source, j):
        return ref[source, 0:1, j : j + 1][0, 0]

    load_ao.wait()
    for j in range(2):
        code = code_of(meta_ref, me, j)
        codes_ref[2 * me + j] = code
        use(outb[2 * me + j], code)

    def take(k, c, source):
        info(2 * k + c, source, source).wait_recv()
        for j in range(2):
            slot(k, c, j, source, source).wait_recv()
            code = code_of(info_ref, source, j)
            codes_ref[2 * source + j] = code
            use(inb[2 * source + j], code)

    take(0, 1, pair)
    keep.wait()
    each(SIDE, 1 + OUT_AHEAD, outward)
    each(0, 1 + ON_AHEAD, onward)
    across(0)

    def arrive(k):
        pl.when(k + TILES_AHEAD <= 15)(lambda: advance(k + TILES_AHEAD))
        pl.when(k + OUT_AHEAD <= 15)(lambda: outward(k + OUT_AHEAD))
        dz, dx = step_of(k)
        for c in range(2):
            take(k, c, shifted(me, (dz, dx, c), -1))
        pl.when(k + ON_AHEAD <= 15)(lambda: onward(k + ON_AHEAD))
        across(k)

    each(1, 16, arrive)

    for b in range(NBAT):
        for f in range(FIELDS):
            mine[pl.ds(b * FIELDS + f, 1), :] = jnp.sum(acc[b, f], axis=0, keepdims=True)
    mine[pl.ds(6, 2), :] = jnp.zeros((2, PTS), jnp.float32)
    total = mine[...]
    swaps = []
    for step in range(1, SIDE):
        copy = pltpu.make_async_remote_copy(
            src_ref=mine, dst_ref=parts.at[step - 1], send_sem=part_send.at[step - 1],
            recv_sem=part_recv.at[step - 1], device_id={"narrow": (row + step) % SIDE},
            device_id_type=MESH,
        )
        copy.start()
        swaps.append(copy)
    info(1, pair, me).wait_send()
    for j in range(2):
        slot(0, 1, j, pair, me).wait_send()

    def drain(k):
        plane(k, pair, me).wait_send()
        for c in range(2):
            info(2 * k + c, pair, me).wait_send()
            for j in range(2):
                slot(k, c, j, pair, me).wait_send()

    def finish(k):
        home = home_of(k)
        for side, way in enumerate((1, -1)):
            spread(block, k, home, side, way).wait_send()
        passed(k, home, row, 1).wait_send()
        paired(k, home).wait_send()
        dz, dx = turn(k)
        paired(k, shifted(me, (dx, dz, 1), -1)).wait_recv()

    each(1, 16, drain)
    each(0, 16, finish)
    for step, copy in enumerate(swaps):
        copy.wait()
        total = total + parts[step]
    dens_ref[...] = total


def dispatch(dest, place, rows, cols, tiles, ao, occ):
    vmem, smem = pl.BlockSpec(memory_space=pltpu.VMEM), pl.BlockSpec(memory_space=pltpu.SMEM)
    dma, hbm = pltpu.SemaphoreType.DMA, pl.BlockSpec(memory_space=pltpu.HBM)
    return pl.pallas_call(
        dispatch_kernel,
        out_shape=(
            jax.ShapeDtypeStruct((8, PTS), jnp.float32),
            jax.ShapeDtypeStruct((2 * NWIDE,), jnp.int32),
            jax.ShapeDtypeStruct((NWIDE * SIDE, NOCC, BLK), jnp.bfloat16),
        ),
        in_specs=[smem, smem, smem, smem, hbm, hbm, hbm],
        out_specs=(vmem, smem, hbm),
        scratch_shapes=[
            pltpu.VMEM((TILES, ROWS, BLK), jnp.bfloat16),
            pltpu.VMEM((NBAT * KB, BLK, PTS), jnp.bfloat16),
            pltpu.VMEM((BLK, NOCC), jnp.bfloat16),
            dma((3,)),
            pltpu.VMEM((NWIDE, 8, BLK), jnp.int32),
            pltpu.VMEM((NWIDE, 8, BLK), jnp.int32),
            pltpu.VMEM((2 * NWIDE, ROWS, BLK), jnp.bfloat16),
            pltpu.VMEM((2 * NWIDE, ROWS, BLK), jnp.bfloat16),
            pltpu.VMEM((NBAT, FIELDS, 8, PTS), jnp.float32),
            pltpu.VMEM((8, PTS), jnp.float32),
            pltpu.VMEM((SIDE - 1, 8, PTS), jnp.float32),
            pltpu.VMEM((NOCC, BLK), jnp.bfloat16),
            dma((NWIDE, 2)), dma((NWIDE, 2)),
            dma((NWIDE,)), dma((NWIDE,)), dma((SIDE - 1,)), dma((SIDE - 1,)),
            dma, dma((16,)), dma((16,)), dma((16, 2)), dma((16, 2)), dma((16,)), dma((16,)),
            dma((16,)), dma((16,)),
        ],
        compiler_params=pltpu.CompilerParams(
            collective_id=0, has_side_effects=True, vmem_limit_bytes=56 * 2**20
        ),
        cost_estimate=pl.CostEstimate(
            flops=70_000_000_000, bytes_accessed=10_000_000, transcendentals=0
        ),
    )(dest, place, rows, cols, tiles, ao, occ)


def respond_kernel(
    code_ref, count_ref, dens_ref, weight_ref, first_ref, second_ref, ao_ref, occ_hbm,
    left_hbm, occ, pot, scaled, answer, total, left, head, follow, occ_sem, left_sem,
):
    load_occ = pltpu.make_async_copy(occ_hbm, occ, occ_sem)
    load_occ.start()

    lane = lax.broadcasted_iota(jnp.int32, (1, PTS), 1)
    for b in range(NBAT):
        scale = jnp.where(lane < count_ref[b], weight_ref[pl.ds(b, 1), :], 0.0)
        one, two = first_ref[pl.ds(b, 1), :], second_ref[pl.ds(b, 1), :]
        d = [dens_ref[pl.ds(b * FIELDS + f, 1), :] for f in range(FIELDS)]
        for f in range(FIELDS):
            p, q = d[(f + 1) % 3], d[(f + 2) % 3]
            pot[pl.ds(b * FIELDS + f, 1), :] = scale * (one * d[f] + two * p * q)

    def blocks(i, carry):
        b, f = i // FIELDS, i % FIELDS
        aos = ao_ref[pl.ds(b * KB, KB)].reshape(KB * BLK, PTS)
        scaled[...] = (aos.astype(jnp.float32) * pot[pl.ds(i, 1), :]).astype(jnp.bfloat16)
        part = lax.dot_general(
            scaled[...], aos, (((1,), (1,)), ((), ())), preferred_element_type=jnp.float32
        ).astype(jnp.bfloat16)
        for a in range(KB):
            for c in range(KB):
                answer[b * 25 + a * KB + c, :, pl.ds(pl.multiple_of(f * BLK, BLK), BLK)] = part[
                    a * BLK : (a + 1) * BLK, c * BLK : (c + 1) * BLK
                ]
        return carry

    lax.fori_loop(0, NBAT * FIELDS, blocks, 0)

    def clear(c, carry):
        head[c] = -1
        follow[2 * c] = -1
        follow[2 * c + 1] = -1
        return carry

    lax.fori_loop(0, 32, clear, 0)

    def link(r, carry):
        code = code_ref[r]
        column = (code // 262144) % 32

        @pl.when((code // 32768) % 2 == 1)
        def _():
            follow[r] = head[column]
            head[column] = r

        return carry

    lax.fori_loop(0, 2 * NWIDE, link, 0)
    load_occ.wait()

    def column_sum(c, carry):
        def term(r):
            code = code_ref[r]
            return occ[(r // 2) * 4 + (code // 65536) % 4], answer[(code // 512) % 64]

        def two(r):
            nxt = follow[r]
            other = jnp.where(nxt >= 0, nxt, r)
            (left_a, right_a), (left_b, right_b) = term(r), term(other)
            right_b = jnp.where(nxt >= 0, right_b, jnp.zeros_like(right_b))
            return jnp.dot(
                jnp.concatenate([left_a, left_b], axis=1),
                jnp.concatenate([right_a, right_b], axis=0), preferred_element_type=jnp.float32,
            )

        def after(r):
            nxt = follow[jnp.maximum(r, 0)]
            last = jnp.logical_or(r < 0, nxt < 0)
            return jnp.where(last, -1, follow[jnp.maximum(nxt, 0)])

        def add(r):
            total[...] += two(r)
            return after(r)

        first = head[c]

        @pl.when(first < 0)
        def _():
            total[...] = jnp.zeros_like(total)

        @pl.when(first >= 0)
        def _():
            total[...] = two(first)

        lax.while_loop(lambda r: r >= 0, add, after(first))
        slot = c % 2

        @pl.when(c >= 2)
        def _():
            pltpu.make_async_copy(left.at[slot], left_hbm.at[c], left_sem.at[slot]).wait()

        for half in range(2):
            for f in range(FIELDS):
                left[slot, pl.ds(half * HALF + f * 256, 256), :] = total[
                    half * 256 : (half + 1) * 256, f * BLK : (f + 1) * BLK
                ].astype(jnp.bfloat16)
        pltpu.make_async_copy(left.at[slot], left_hbm.at[c], left_sem.at[slot]).start()
        return carry

    lax.fori_loop(0, 32, column_sum, 0)
    for slot in range(2):
        pltpu.make_async_copy(left.at[slot], left_hbm.at[slot], left_sem.at[slot]).wait()


def respond(codes, counts, dens, weights, first, second, ao, occ):
    vmem, smem = pl.BlockSpec(memory_space=pltpu.VMEM), pl.BlockSpec(memory_space=pltpu.SMEM)
    hbm = pl.BlockSpec(memory_space=pltpu.HBM)
    return pl.pallas_call(
        respond_kernel,
        out_shape=jax.ShapeDtypeStruct((32, 2 * HALF, BLK), jnp.bfloat16),
        in_specs=[smem, smem, vmem, vmem, vmem, vmem, vmem, hbm],
        out_specs=hbm,
        scratch_shapes=[
            pltpu.VMEM((128, NOCC, BLK), jnp.bfloat16),
            pltpu.VMEM((8, PTS), jnp.float32),
            pltpu.VMEM((KB * BLK, PTS), jnp.bfloat16),
            pltpu.VMEM((50, BLK, ROWS), jnp.bfloat16),
            pltpu.VMEM((NOCC, ROWS), jnp.float32),
            pltpu.VMEM((2, 2 * HALF, BLK), jnp.bfloat16),
            pltpu.SMEM((32,), jnp.int32),
            pltpu.SMEM((64,), jnp.int32),
            pltpu.SemaphoreType.DMA,
            pltpu.SemaphoreType.DMA((2,)),
        ],
        compiler_params=pltpu.CompilerParams(vmem_limit_bytes=62 * 2**20),
        cost_estimate=pl.CostEstimate(
            flops=30_000_000_000, bytes_accessed=30_000_000, transcendentals=0
        ),
    )(codes, counts, dens, weights, first, second, ao, occ)


def reduce_kernel(
    left_hbm, vir_hbm, out_ref, left, vir, give, got, mid, y_one, x_one, y_sum, x_sum, x_two, y_two,
    left_sem, vir_sem, give_send, give_recv, y_one_send, y_one_recv, x_one_send, x_one_recv,
    x_two_send, x_two_recv, y_two_send, y_two_recv,
):
    me = lax.axis_index("wide")
    row = lax.axis_index("narrow")
    core, chip = me % 2, me // 2
    pair = shifted(me, (0, 0, 1))
    peers = [shifted(me, (z, x, 0)) for z, x in CHIPS]
    barrier = pltpu.get_barrier_semaphore()
    for peer in [pair, *peers]:
        pl.semaphore_signal(barrier, inc=1, device_id={"wide": peer}, device_id_type=MESH)
    for step in range(1, SIDE):
        pl.semaphore_signal(
            barrier, inc=1, device_id={"narrow": (row + step) % SIDE}, device_id_type=MESH
        )

    def load(half, c):
        rows = pl.ds(pl.multiple_of(half * HALF, HALF), HALF)
        return pltpu.make_async_copy(
            left_hbm.at[c, rows],
            left.at[half, :, pl.ds(pl.multiple_of(c * BLK, BLK), BLK)],
            left_sem.at[half, c],
        )

    def load_vir(q):
        return pltpu.make_async_copy(
            vir_hbm.at[:, pl.ds(pl.multiple_of(q * 256, 256), 256)], vir.at[q], vir_sem.at[q]
        )

    def each(last, step):
        def run(k, carry):
            step(k)
            return carry

        lax.fori_loop(0, last, run, 0)

    order = [(row + 1 + i) % SIDE for i in range(SIDE)]
    load_vir(order[0]).start()
    each(32, lambda c: load(1 - core, c).start())
    load_vir(order[1]).start()
    each(32, lambda c: load(core, c).start())
    for q in order[2:]:
        load_vir(q).start()
    pl.semaphore_wait(barrier, 1 + len(peers) + SIDE - 1)

    def to(axis, peer, src, dst, ssem, rsem):
        return pltpu.make_async_remote_copy(
            src_ref=src, dst_ref=dst, send_sem=ssem, recv_sem=rsem, device_id={axis: peer},
            device_id_type=MESH,
        )

    def product(half, q):
        return jnp.dot(left[half], vir[q], preferred_element_type=jnp.float32).reshape(
            FIELDS, 256, 256
        )

    def hand(q):
        return to("wide", pair, give.at[q], got.at[q], give_send.at[q], give_recv.at[q])

    def other_half(q):
        load_vir(q).wait()
        give[q] = product(1 - core, q).astype(jnp.bfloat16)
        hand(q).start()

    def down(q, y):
        return to(
            "narrow", q, mid.at[q, :, :, pl.ds(0, BLK)], y_one.at[y], y_one_send.at[q],
            y_one_recv.at[y],
        )

    def over(q, k, peer):
        rows = pl.ds(pl.multiple_of((peer // 2) * 16, 16), 16)
        return to(
            "wide", peer, mid.at[q, :, rows, pl.ds(BLK, BLK)], x_one.at[k, q],
            x_one_send.at[k, q], x_one_recv.at[k, q],
        )

    def own_half(q):
        own = product(core, q)
        hand(q).wait_recv()
        mid[q] = (own + got[q].astype(jnp.float32)).astype(jnp.bfloat16)
        pl.when(q != row)(lambda: down(q, row).start())
        for k, peer in enumerate(peers):
            over(q, k, peer).start()

    each(32, lambda c: load(1 - core, c).wait())
    other_half(order[0])
    each(32, lambda c: load(core, c).wait())

    def both(i):
        pl.when(i < SIDE - 1)(lambda: other_half((row + 2 + i) % SIDE))
        own_half((row + 1 + i) % SIDE)

    each(SIDE, both)
    here = pl.ds(pl.multiple_of(chip * 16, 16), 16)

    total = mid[row, :, :, pl.ds(0, BLK)].astype(jnp.float32)
    for step in range(1, SIDE):
        y = (row + step) % SIDE
        down(y, y).wait_recv()
        total = total + y_one[y].astype(jnp.float32)
    y_sum[...] = total.astype(jnp.bfloat16)

    def scatter(k, peer):
        rows = pl.ds(pl.multiple_of((peer // 2) * 16, 16), 16)
        return to("wide", peer, y_sum.at[:, rows], x_two.at[k], x_two_send.at[k], x_two_recv.at[k])

    for k, peer in enumerate(peers):
        scatter(k, peer).start()

    total = mid[:, :, here, pl.ds(BLK, BLK)].astype(jnp.float32)
    for k, peer in enumerate(peers):
        for q in range(SIDE):
            over(q, k, peer).wait_recv()
        total = total + x_one[k].astype(jnp.float32)
    x_sum[...] = total.astype(jnp.bfloat16)

    def give_row(step):
        y = (row + step) % SIDE
        return to(
            "narrow", y, x_sum.at[y], y_two.at[step - 1], y_two_send.at[step - 1],
            y_two_recv.at[step - 1],
        )

    for step in range(1, SIDE):
        give_row(step).start()

    total = y_sum[:, here].astype(jnp.float32)
    for k, peer in enumerate(peers):
        scatter(k, peer).wait_recv()
        total = total + x_two[k].astype(jnp.float32)
    out_ref[:, :, pl.ds(0, BLK)] = total
    total = x_sum[row].astype(jnp.float32)
    for step in range(1, SIDE):
        give_row(step).wait_recv()
        total = total + y_two[step - 1].astype(jnp.float32)
    out_ref[:, :, pl.ds(BLK, BLK)] = total

    def sent(q):
        hand(q).wait_send()
        pl.when(q != row)(lambda: down(q, row).wait_send())
        for k, peer in enumerate(peers):
            over(q, k, peer).wait_send()

    each(SIDE, sent)
    for k, peer in enumerate(peers):
        scatter(k, peer).wait_send()
    for step in range(1, SIDE):
        give_row(step).wait_send()


def reduced(left, vir):
    hbm = pl.BlockSpec(memory_space=pltpu.HBM)
    dma, bf16 = pltpu.SemaphoreType.DMA, jnp.bfloat16
    chips = len(CHIPS)
    return pl.pallas_call(
        reduce_kernel,
        out_shape=jax.ShapeDtypeStruct((FIELDS, 16, 256), jnp.float32),
        in_specs=[hbm, hbm],
        out_specs=pl.BlockSpec(memory_space=pltpu.VMEM),
        scratch_shapes=[
            pltpu.VMEM((2, HALF, 4096), bf16),
            pltpu.VMEM((SIDE, 4096, 256), bf16),
            pltpu.VMEM((SIDE, FIELDS, 256, 256), bf16),
            pltpu.VMEM((SIDE, FIELDS, 256, 256), bf16),
            pltpu.VMEM((SIDE, FIELDS, 256, 256), bf16),
            pltpu.VMEM((SIDE, FIELDS, 256, BLK), bf16),
            pltpu.VMEM((chips, SIDE, FIELDS, 16, BLK), bf16),
            pltpu.VMEM((FIELDS, 256, BLK), bf16),
            pltpu.VMEM((SIDE, FIELDS, 16, BLK), bf16),
            pltpu.VMEM((chips, FIELDS, 16, BLK), bf16),
            pltpu.VMEM((SIDE - 1, FIELDS, 16, BLK), bf16),
            dma((2, 32)), dma((SIDE,)), dma((SIDE,)), dma((SIDE,)), dma((SIDE,)), dma((SIDE,)),
            dma((chips, SIDE)), dma((chips, SIDE)), dma((chips,)), dma((chips,)),
            dma((SIDE - 1,)), dma((SIDE - 1,)),
        ],
        compiler_params=pltpu.CompilerParams(
            collective_id=1, has_side_effects=True, vmem_limit_bytes=50 * 2**20
        ),
        cost_estimate=pl.CostEstimate(
            flops=30_000_000_000, bytes_accessed=30_000_000, transcendentals=0
        ),
    )(left, vir)


def body(
    dens_tiles,
    tile_dest,
    tile_place,
    tile_rows,
    tile_cols,
    ao_values,
    point_count,
    weights,
    kernel_first,
    kernel_second,
    occ_coef,
    vir_coef,
):
    ao = ao_values.reshape(NBAT * KB, BLK, PTS)
    dens, codes, occ_all = dispatch(
        tile_dest.T, tile_place.T, tile_rows, tile_cols,
        dens_tiles.reshape(TILES, ROWS, BLK), ao, occ_coef,
    )
    left = respond(
        codes, point_count, dens, weights, kernel_first, kernel_second, ao,
        occ_all,
    )
    return reduced(left, vir_coef)


def solution(mesh):
    in_specs = (
        P(("wide", "narrow"), None, None, None),
        P(("wide", "narrow"), None),
        P(("wide", "narrow"), None),
        P(("wide", "narrow")),
        P(("wide", "narrow")),
        P("wide", None, None),
        P("wide"),
        P("wide", None),
        P("wide", None),
        P("wide", None),
        P("wide", None),
        P("narrow", None),
    )
    out_specs = P(None, "wide", "narrow")
    return jax.shard_map(body, mesh=mesh, in_specs=in_specs, out_specs=out_specs, check_vma=False)
```

```python
import jax
import jax.numpy as jnp
from jax import lax
from jax.experimental import pallas as pl
from jax.experimental.pallas import tpu as pltpu
from jax.sharding import PartitionSpec as P

NOCC = 512
NVIR = 1024
BLK = 128
KB = 5
FIELDS = 3
NBAT = 2
PTS = 1280
SIDE = 4
NWIDE = 32
TILES = 16
SLOTS = 8
ROWS = FIELDS * BLK
HALF = FIELDS * NOCC // 2
MESH = pl.DeviceIdType.MESH
CHIPS = [(2, 2), (1, 1), (3, 3), (1, 3), (3, 1), (1, 2), (3, 2), (2, 1), (2, 3), (0, 2), (2, 0), (0, 1), (0, 3), (1, 0), (3, 0)]
OUT_AHEAD, TILES_AHEAD, ON_AHEAD = 11, 8, 7
OFFSETS = [(z, x, c) for z, x in CHIPS for c in range(2)] + [(0, 0, 1)]


def shifted(me, offset, sign=1):
    z, x, c = me // 8, (me // 2) % 4, me % 2
    z = (z + sign * offset[0] + 2 * SIDE) % SIDE
    x = (x + sign * offset[1] + 2 * SIDE) % SIDE
    c = (c + offset[2]) % 2
    return z * 8 + x * 2 + c


def dispatch_kernel(
    dest_ref, place_ref, rows_ref, cols_ref, tiles_hbm, ao_hbm, occ_hbm, dens_ref, codes_ref, all_ref,
    tiles_ref, ao_ref, occ_ref, load_sem, meta_ref, info_ref, outb, inb, acc, mine, parts, block,
    send_sem, recv_sem, meta_send, meta_recv, part_send, part_recv,
    own_sem, plane_send, plane_recv, side_send, side_recv, pass_send, pass_recv, pair_send, pair_recv,
):
    me = lax.axis_index("wide")
    row = lax.axis_index("narrow")
    quarter = pl.ds(pl.multiple_of(row * BLK, BLK), BLK)
    load_occ = pltpu.make_async_copy(occ_hbm.at[quarter], occ_ref, load_sem.at[0])
    load_tiles = pltpu.make_async_copy(tiles_hbm, tiles_ref, load_sem.at[1])
    load_ao = pltpu.make_async_copy(ao_hbm, ao_ref, load_sem.at[2])
    load_occ.start()
    load_tiles.start()
    load_ao.start()
    barrier = pltpu.get_barrier_semaphore()
    for offset in OFFSETS:
        pl.semaphore_signal(
            barrier, inc=1, device_id={"wide": shifted(me, offset)}, device_id_type=MESH
        )
    for step in range(1, SIDE):
        pl.semaphore_signal(
            barrier, inc=1, device_id={"narrow": (row + step) % SIDE}, device_id_type=MESH
        )

    load_occ.wait()
    turned = occ_ref[...].T
    for w in range(NWIDE):
        block[pl.ds((w % 2) * 256 + (w // 2) * 16, 16), :] = turned[w * 16 : (w + 1) * 16]

    acc[...] = jnp.zeros_like(acc)
    pl.semaphore_wait(barrier, len(OFFSETS) + SIDE - 1)

    def step_of(k):
        dz = sum(jnp.where(k == n + 1, z, 0) for n, (z, _) in enumerate(CHIPS))
        dx = sum(jnp.where(k == n + 1, x, 0) for n, (_, x) in enumerate(CHIPS))
        return dz, dx

    core = me % 2

    def turn(k):
        d, e = k % 4, k // 4
        return e + core * (d - e), d + core * (e - d)

    def home_of(k):
        return shifted(me, (*turn(k), 0), -1)

    def slot(k, c, j, peer, source):
        return pltpu.make_async_remote_copy(
            src_ref=outb.at[2 * peer + j], dst_ref=inb.at[2 * source + j],
            send_sem=send_sem.at[2 * k + c, j], recv_sem=recv_sem.at[2 * k + c, j],
            device_id={"wide": peer}, device_id_type=MESH,
        )

    def info(k, peer, source):
        return pltpu.make_async_remote_copy(
            src_ref=meta_ref.at[peer], dst_ref=info_ref.at[source], send_sem=meta_send.at[k],
            recv_sem=meta_recv.at[k], device_id={"wide": peer}, device_id_type=MESH,
        )

    def send_tiles(k):
        dz, dx = step_of(k)
        for c in range(2):
            info(2 * k + c, shifted(me, (dz, dx, c)), me).start()
            for j in range(2):
                slot(k, c, j, shifted(me, (dz, dx, c)), me).start()

    def place(home, y):
        return all_ref.at[home * SIDE + (y + 2 * SIDE) % SIDE]

    def plane(k, peer, home, src=block):
        return pltpu.make_async_remote_copy(
            src_ref=src, dst_ref=place(home, row), send_sem=plane_send.at[k],
            recv_sem=plane_recv.at[k], device_id={"wide": peer}, device_id_type=MESH,
        )

    def send_block(k):
        plane(k, shifted(me, (*turn(k), 0)), me).start()

    def spread(src, k, home, side, way):
        return pltpu.make_async_remote_copy(
            src_ref=src, dst_ref=place(home, row), send_sem=side_send.at[k, side],
            recv_sem=side_recv.at[k, side], device_id={"narrow": (row + way + SIDE) % SIDE},
            device_id_type=MESH,
        )

    def passed(k, home, y, way):
        return pltpu.make_async_remote_copy(
            src_ref=place(home, y), dst_ref=place(home, y), send_sem=pass_send.at[k],
            recv_sem=pass_recv.at[k], device_id={"narrow": (row + way + SIDE) % SIDE},
            device_id_type=MESH,
        )

    def paired(k, home):
        four = all_ref.at[pl.ds(home * SIDE, SIDE)]
        return pltpu.make_async_remote_copy(
            src_ref=four, dst_ref=four, send_sem=pair_send.at[k], recv_sem=pair_recv.at[k],
            device_id={"wide": shifted(me, (0, 0, 1))}, device_id_type=MESH,
        )

    def outward(k):
        home = home_of(k)
        plane(k, home, home).wait_recv()
        for side, way in enumerate((1, -1)):
            spread(place(home, row), k, home, side, way).start()

    def forward(k):
        home = home_of(k)
        for e in range(1, SIDE):
            plane(
                4 * e + k, shifted(me, (*turn(4 * e), 0)), home, place(home, row)
            ).start()

    def onward(k):
        home = home_of(k)
        for side, way in enumerate((1, -1)):
            pltpu.make_async_remote_copy(
                src_ref=block, dst_ref=place(home, row - way), send_sem=side_send.at[k, side],
                recv_sem=side_recv.at[k, side], device_id={"narrow": (row - way + SIDE) % SIDE},
                device_id_type=MESH,
            ).wait_recv()
        way = 1 - 2 * (k % 2)
        passed(k, home, row - way, way).start()

    def across(k):
        home = home_of(k)
        passed(k, home, row + 2, 1).wait_recv()
        paired(k, home).start()

    def each(first, last, step):
        def run(k, carry):
            step(k)
            return carry

        lax.fori_loop(first, last, run, 0)

    keep = pltpu.make_async_copy(block, place(me, row), own_sem)
    keep.start()
    for side, way in enumerate((1, -1)):
        spread(block, 0, me, side, way).start()
    pair = shifted(me, (0, 0, 1))
    for k in (1, 2, 3, 4, 8, 12):
        send_block(k)
    load_tiles.wait()
    lane = lax.broadcasted_iota(jnp.int32, (8, BLK), 1)

    def route(peer):
        found = [-1, -1]
        for r in range(2 * TILES):
            hit = dest_ref[r % 2, r // 2] == peer
            found = [
                jnp.where(jnp.logical_and(hit, found[0] < 0), r, found[0]),
                jnp.where(jnp.logical_and(hit, found[0] >= 0), r, found[1]),
            ]
        codes = []
        for j in range(2):
            r = jnp.maximum(found[j], 0)
            t = r // 2
            spot = place_ref[r % 2, t]
            batch, block_pair = spot // 25, spot % 25
            code = (
                (batch * KB + block_pair // KB) + 16 * (batch * KB + block_pair % KB) + 256 * batch
                + 512 * spot + 32768 + 65536 * rows_ref[t] + 262144 * cols_ref[t]
            )
            codes.append(jnp.where(found[j] >= 0, code, 0))
            outb[2 * peer + j] = tiles_ref[t]
        meta_ref[peer] = jnp.where(lane == 0, codes[0], jnp.where(lane == 1, codes[1], 0))

    def route_chip(k):
        dz, dx = step_of(k)
        for c in range(2):
            route(shifted(me, (dz, dx, c)))

    def advance(k):
        pl.when(k < 15)(lambda: route_chip(k + 1))
        send_tiles(k)

    route(pair)
    route(me)
    route_chip(1)
    info(1, pair, me).start()
    for j in range(2):
        slot(0, 1, j, pair, me).start()
    advance(1)

    def relay(k):
        outward(k)
        forward(k)

    each(1, SIDE, relay)
    each(2, 1 + TILES_AHEAD, advance)

    def use(tile, code):
        first, second = code % 16, (code // 16) % 16
        batch, valid = (code // 256) % 2, (code // 32768) % 2
        lives = [jnp.logical_and(valid == 1, batch == b) for b in range(NBAT)]
        for q in range(PTS // 256):
            cols = pl.ds(q * 256, 256)
            mixed = jnp.dot(tile, ao_ref[second, :, cols], preferred_element_type=jnp.float32)
            left = ao_ref[first, :, cols].astype(jnp.float32)
            part = jnp.sum(
                mixed.reshape(FIELDS, BLK // 8, 8, 256) * left.reshape(1, BLK // 8, 8, 256), axis=1
            )
            for b in range(NBAT):
                acc[b, :, :, cols] += jnp.where(lives[b], part, 0.0)

    def code_of(ref, source, j):
        return ref[source, 0:1, j : j + 1][0, 0]

    load_ao.wait()
    for j in range(2):
        code = code_of(meta_ref, me, j)
        codes_ref[2 * me + j] = code
        use(outb[2 * me + j], code)

    def take(k, c, source):
        info(2 * k + c, source, source).wait_recv()
        for j in range(2):
            slot(k, c, j, source, source).wait_recv()
            code = code_of(info_ref, source, j)
            codes_ref[2 * source + j] = code
            use(inb[2 * source + j], code)

    take(0, 1, pair)
    keep.wait()
    each(SIDE, 1 + OUT_AHEAD, outward)
    each(0, 1 + ON_AHEAD, onward)
    across(0)

    def arrive(k):
        pl.when(k + TILES_AHEAD <= 15)(lambda: advance(k + TILES_AHEAD))
        pl.when(k + OUT_AHEAD <= 15)(lambda: outward(k + OUT_AHEAD))
        dz, dx = step_of(k)
        for c in range(2):
            take(k, c, shifted(me, (dz, dx, c), -1))
        pl.when(k + ON_AHEAD <= 15)(lambda: onward(k + ON_AHEAD))
        across(k)

    each(1, 16, arrive)

    for b in range(NBAT):
        for f in range(FIELDS):
            mine[pl.ds(b * FIELDS + f, 1), :] = jnp.sum(acc[b, f], axis=0, keepdims=True)
    mine[pl.ds(6, 2), :] = jnp.zeros((2, PTS), jnp.float32)
    total = mine[...]
    swaps = []
    for step in range(1, SIDE):
        copy = pltpu.make_async_remote_copy(
            src_ref=mine, dst_ref=parts.at[step - 1], send_sem=part_send.at[step - 1],
            recv_sem=part_recv.at[step - 1], device_id={"narrow": (row + step) % SIDE},
            device_id_type=MESH,
        )
        copy.start()
        swaps.append(copy)
    info(1, pair, me).wait_send()
    for j in range(2):
        slot(0, 1, j, pair, me).wait_send()

    def drain(k):
        plane(k, pair, me).wait_send()
        for c in range(2):
            info(2 * k + c, pair, me).wait_send()
            for j in range(2):
                slot(k, c, j, pair, me).wait_send()

    def finish(k):
        home = home_of(k)
        for side, way in enumerate((1, -1)):
            spread(block, k, home, side, way).wait_send()
        passed(k, home, row, 1).wait_send()
        paired(k, home).wait_send()
        dz, dx = turn(k)
        paired(k, shifted(me, (dx, dz, 1), -1)).wait_recv()

    each(1, 16, drain)
    each(0, 16, finish)
    for step, copy in enumerate(swaps):
        copy.wait()
        total = total + parts[step]
    dens_ref[...] = total


def dispatch(dest, place, rows, cols, tiles, ao, occ):
    vmem, smem = pl.BlockSpec(memory_space=pltpu.VMEM), pl.BlockSpec(memory_space=pltpu.SMEM)
    dma, hbm = pltpu.SemaphoreType.DMA, pl.BlockSpec(memory_space=pltpu.HBM)
    return pl.pallas_call(
        dispatch_kernel,
        out_shape=(
            jax.ShapeDtypeStruct((8, PTS), jnp.float32),
            jax.ShapeDtypeStruct((2 * NWIDE,), jnp.int32),
            jax.ShapeDtypeStruct((NWIDE * SIDE, NOCC, BLK), jnp.bfloat16),
        ),
        in_specs=[smem, smem, smem, smem, hbm, hbm, hbm],
        out_specs=(vmem, smem, hbm),
        scratch_shapes=[
            pltpu.VMEM((TILES, ROWS, BLK), jnp.bfloat16),
            pltpu.VMEM((NBAT * KB, BLK, PTS), jnp.bfloat16),
            pltpu.VMEM((BLK, NOCC), jnp.bfloat16),
            dma((3,)),
            pltpu.VMEM((NWIDE, 8, BLK), jnp.int32),
            pltpu.VMEM((NWIDE, 8, BLK), jnp.int32),
            pltpu.VMEM((2 * NWIDE, ROWS, BLK), jnp.bfloat16),
            pltpu.VMEM((2 * NWIDE, ROWS, BLK), jnp.bfloat16),
            pltpu.VMEM((NBAT, FIELDS, 8, PTS), jnp.float32),
            pltpu.VMEM((8, PTS), jnp.float32),
            pltpu.VMEM((SIDE - 1, 8, PTS), jnp.float32),
            pltpu.VMEM((NOCC, BLK), jnp.bfloat16),
            dma((NWIDE, 2)), dma((NWIDE, 2)),
            dma((NWIDE,)), dma((NWIDE,)), dma((SIDE - 1,)), dma((SIDE - 1,)),
            dma, dma((16,)), dma((16,)), dma((16, 2)), dma((16, 2)), dma((16,)), dma((16,)),
            dma((16,)), dma((16,)),
        ],
        compiler_params=pltpu.CompilerParams(
            collective_id=0, has_side_effects=True, vmem_limit_bytes=56 * 2**20
        ),
        cost_estimate=pl.CostEstimate(
            flops=70_000_000_000, bytes_accessed=10_000_000, transcendentals=0
        ),
    )(dest, place, rows, cols, tiles, ao, occ)


def respond_kernel(
    code_ref, count_ref, dens_ref, weight_ref, first_ref, second_ref, ao_ref, occ_hbm,
    left_hbm, occ, pot, scaled, answer, total, left, head, follow, occ_sem, left_sem,
):
    loads = [
        pltpu.make_async_copy(occ_hbm.at[pl.ds(i * 8, 8)], occ.at[pl.ds(i * 8, 8)], occ_sem.at[i])
        for i in range(16)
    ]
    for load in loads:
        load.start()

    lane = lax.broadcasted_iota(jnp.int32, (1, PTS), 1)
    for b in range(NBAT):
        scale = jnp.where(lane < count_ref[b], weight_ref[pl.ds(b, 1), :], 0.0)
        one, two = first_ref[pl.ds(b, 1), :], second_ref[pl.ds(b, 1), :]
        d = [dens_ref[pl.ds(b * FIELDS + f, 1), :] for f in range(FIELDS)]
        for f in range(FIELDS):
            p, q = d[(f + 1) % 3], d[(f + 2) % 3]
            pot[pl.ds(b * FIELDS + f, 1), :] = scale * (one * d[f] + two * p * q)

    def blocks(i, carry):
        b, f = i // FIELDS, i % FIELDS
        aos = ao_ref[pl.ds(b * KB, KB)].reshape(KB * BLK, PTS)
        scaled[...] = (aos.astype(jnp.float32) * pot[pl.ds(i, 1), :]).astype(jnp.bfloat16)
        part = lax.dot_general(
            scaled[...], aos, (((1,), (1,)), ((), ())), preferred_element_type=jnp.float32
        ).astype(jnp.bfloat16)
        for a in range(KB):
            for c in range(KB):
                answer[b * 25 + a * KB + c, :, pl.ds(pl.multiple_of(f * BLK, BLK), BLK)] = part[
                    a * BLK : (a + 1) * BLK, c * BLK : (c + 1) * BLK
                ]
        return carry

    lax.fori_loop(0, NBAT * FIELDS, blocks, 0)

    def clear(c, carry):
        head[c] = -1
        follow[2 * c] = -1
        follow[2 * c + 1] = -1
        return carry

    lax.fori_loop(0, 32, clear, 0)

    def link(r, carry):
        code = code_ref[r]
        column = (code // 262144) % 32

        @pl.when((code // 32768) % 2 == 1)
        def _():
            follow[r] = head[column]
            head[column] = r

        return carry

    lax.fori_loop(0, 2 * NWIDE, link, 0)
    for load in loads:
        load.wait()

    def column_sum(c, carry):
        def term(r):
            code = code_ref[r]
            return occ[(r // 2) * 4 + (code // 65536) % 4], answer[(code // 512) % 64]

        def two(r):
            nxt = follow[r]
            other = jnp.where(nxt >= 0, nxt, r)
            (left_a, right_a), (left_b, right_b) = term(r), term(other)
            right_b = jnp.where(nxt >= 0, right_b, jnp.zeros_like(right_b))
            return jnp.dot(
                jnp.concatenate([left_a, left_b], axis=1),
                jnp.concatenate([right_a, right_b], axis=0), preferred_element_type=jnp.float32,
            )

        def after(r):
            nxt = follow[jnp.maximum(r, 0)]
            last = jnp.logical_or(r < 0, nxt < 0)
            return jnp.where(last, -1, follow[jnp.maximum(nxt, 0)])

        def add(r):
            total[...] += two(r)
            return after(r)

        first = head[c]

        @pl.when(first < 0)
        def _():
            total[...] = jnp.zeros_like(total)

        @pl.when(first >= 0)
        def _():
            total[...] = two(first)

        lax.while_loop(lambda r: r >= 0, add, after(first))
        slot = c % SLOTS

        @pl.when(c >= SLOTS)
        def _():
            pltpu.make_async_copy(left.at[slot], left_hbm.at[c], left_sem.at[slot]).wait()

        for half in range(2):
            for f in range(FIELDS):
                left[slot, pl.ds(half * HALF + f * 256, 256), :] = total[
                    half * 256 : (half + 1) * 256, f * BLK : (f + 1) * BLK
                ].astype(jnp.bfloat16)
        pltpu.make_async_copy(left.at[slot], left_hbm.at[c], left_sem.at[slot]).start()
        return carry

    lax.fori_loop(0, 32, column_sum, 0)
    for slot in range(SLOTS):
        pltpu.make_async_copy(left.at[slot], left_hbm.at[slot], left_sem.at[slot]).wait()


def respond(codes, counts, dens, weights, first, second, ao, occ):
    vmem, smem = pl.BlockSpec(memory_space=pltpu.VMEM), pl.BlockSpec(memory_space=pltpu.SMEM)
    hbm = pl.BlockSpec(memory_space=pltpu.HBM)
    return pl.pallas_call(
        respond_kernel,
        out_shape=jax.ShapeDtypeStruct((32, 2 * HALF, BLK), jnp.bfloat16),
        in_specs=[smem, smem, vmem, vmem, vmem, vmem, vmem, hbm],
        out_specs=hbm,
        scratch_shapes=[
            pltpu.VMEM((128, NOCC, BLK), jnp.bfloat16),
            pltpu.VMEM((8, PTS), jnp.float32),
            pltpu.VMEM((KB * BLK, PTS), jnp.bfloat16),
            pltpu.VMEM((50, BLK, ROWS), jnp.bfloat16),
            pltpu.VMEM((NOCC, ROWS), jnp.float32),
            pltpu.VMEM((SLOTS, 2 * HALF, BLK), jnp.bfloat16),
            pltpu.SMEM((32,), jnp.int32),
            pltpu.SMEM((64,), jnp.int32),
            pltpu.SemaphoreType.DMA((16,)),
            pltpu.SemaphoreType.DMA((SLOTS,)),
        ],
        compiler_params=pltpu.CompilerParams(vmem_limit_bytes=62 * 2**20),
        cost_estimate=pl.CostEstimate(
            flops=30_000_000_000, bytes_accessed=30_000_000, transcendentals=0
        ),
    )(codes, counts, dens, weights, first, second, ao, occ)


def reduce_kernel(
    left_hbm, vir_hbm, out_ref, left, vir, give, got, mid, y_one, x_one, y_sum, x_sum, x_two, y_two,
    left_sem, vir_sem, give_send, give_recv, y_one_send, y_one_recv, x_one_send, x_one_recv,
    x_two_send, x_two_recv, y_two_send, y_two_recv,
):
    me = lax.axis_index("wide")
    row = lax.axis_index("narrow")
    core, chip = me % 2, me // 2
    pair = shifted(me, (0, 0, 1))
    peers = [shifted(me, (z, x, 0)) for z, x in CHIPS]
    barrier = pltpu.get_barrier_semaphore()
    for peer in [pair, *peers]:
        pl.semaphore_signal(barrier, inc=1, device_id={"wide": peer}, device_id_type=MESH)
    for step in range(1, SIDE):
        pl.semaphore_signal(
            barrier, inc=1, device_id={"narrow": (row + step) % SIDE}, device_id_type=MESH
        )

    def load(half, c):
        rows = pl.ds(pl.multiple_of(half * HALF, HALF), HALF)
        return pltpu.make_async_copy(
            left_hbm.at[c, rows],
            left.at[half, :, pl.ds(pl.multiple_of(c * BLK, BLK), BLK)],
            left_sem.at[half, c],
        )

    def load_vir(q):
        return pltpu.make_async_copy(
            vir_hbm.at[:, pl.ds(pl.multiple_of(q * 256, 256), 256)], vir.at[q], vir_sem.at[q]
        )

    def each(last, step):
        def run(k, carry):
            step(k)
            return carry

        lax.fori_loop(0, last, run, 0)

    order = [(row + 1 + i) % SIDE for i in range(SIDE)]
    load_vir(order[0]).start()
    each(32, lambda c: load(1 - core, c).start())
    load_vir(order[1]).start()
    each(32, lambda c: load(core, c).start())
    for q in order[2:]:
        load_vir(q).start()
    pl.semaphore_wait(barrier, 1 + len(peers) + SIDE - 1)

    def to(axis, peer, src, dst, ssem, rsem):
        return pltpu.make_async_remote_copy(
            src_ref=src, dst_ref=dst, send_sem=ssem, recv_sem=rsem, device_id={axis: peer},
            device_id_type=MESH,
        )

    def product(half, q):
        return jnp.dot(left[half], vir[q], preferred_element_type=jnp.float32).reshape(
            FIELDS, 256, 256
        )

    def hand(q):
        return to("wide", pair, give.at[q], got.at[q], give_send.at[q], give_recv.at[q])

    def other_half(q):
        load_vir(q).wait()
        give[q] = product(1 - core, q).astype(jnp.bfloat16)
        hand(q).start()

    def down(q, y):
        return to(
            "narrow", q, mid.at[q, :, :, pl.ds(0, BLK)], y_one.at[y], y_one_send.at[q],
            y_one_recv.at[y],
        )

    def over(q, k, peer):
        rows = pl.ds(pl.multiple_of((peer // 2) * 16, 16), 16)
        return to(
            "wide", peer, mid.at[q, :, rows, pl.ds(BLK, BLK)], x_one.at[k, q],
            x_one_send.at[k, q], x_one_recv.at[k, q],
        )

    def own_half(q):
        own = product(core, q)
        hand(q).wait_recv()
        mid[q] = (own + got[q].astype(jnp.float32)).astype(jnp.bfloat16)
        pl.when(q != row)(lambda: down(q, row).start())
        for k, peer in enumerate(peers):
            over(q, k, peer).start()

    each(32, lambda c: load(1 - core, c).wait())
    other_half(order[0])
    each(32, lambda c: load(core, c).wait())

    def both(i):
        pl.when(i < SIDE - 1)(lambda: other_half((row + 2 + i) % SIDE))
        own_half((row + 1 + i) % SIDE)

    each(SIDE, both)
    here = pl.ds(pl.multiple_of(chip * 16, 16), 16)

    total = mid[row, :, :, pl.ds(0, BLK)].astype(jnp.float32)
    for step in range(1, SIDE):
        y = (row + step) % SIDE
        down(y, y).wait_recv()
        total = total + y_one[y].astype(jnp.float32)
    y_sum[...] = total.astype(jnp.bfloat16)

    def scatter(k, peer):
        rows = pl.ds(pl.multiple_of((peer // 2) * 16, 16), 16)
        return to("wide", peer, y_sum.at[:, rows], x_two.at[k], x_two_send.at[k], x_two_recv.at[k])

    for k, peer in enumerate(peers):
        scatter(k, peer).start()

    total = mid[:, :, here, pl.ds(BLK, BLK)].astype(jnp.float32)
    for k, peer in enumerate(peers):
        for q in range(SIDE):
            over(q, k, peer).wait_recv()
        total = total + x_one[k].astype(jnp.float32)
    x_sum[...] = total.astype(jnp.bfloat16)

    def give_row(step):
        y = (row + step) % SIDE
        return to(
            "narrow", y, x_sum.at[y], y_two.at[step - 1], y_two_send.at[step - 1],
            y_two_recv.at[step - 1],
        )

    for step in range(1, SIDE):
        give_row(step).start()

    total = y_sum[:, here].astype(jnp.float32)
    for k, peer in enumerate(peers):
        scatter(k, peer).wait_recv()
        total = total + x_two[k].astype(jnp.float32)
    out_ref[:, :, pl.ds(0, BLK)] = total
    total = x_sum[row].astype(jnp.float32)
    for step in range(1, SIDE):
        give_row(step).wait_recv()
        total = total + y_two[step - 1].astype(jnp.float32)
    out_ref[:, :, pl.ds(BLK, BLK)] = total

    def sent(q):
        hand(q).wait_send()
        pl.when(q != row)(lambda: down(q, row).wait_send())
        for k, peer in enumerate(peers):
            over(q, k, peer).wait_send()

    each(SIDE, sent)
    for k, peer in enumerate(peers):
        scatter(k, peer).wait_send()
    for step in range(1, SIDE):
        give_row(step).wait_send()


def reduced(left, vir):
    hbm = pl.BlockSpec(memory_space=pltpu.HBM)
    dma, bf16 = pltpu.SemaphoreType.DMA, jnp.bfloat16
    chips = len(CHIPS)
    return pl.pallas_call(
        reduce_kernel,
        out_shape=jax.ShapeDtypeStruct((FIELDS, 16, 256), jnp.float32),
        in_specs=[hbm, hbm],
        out_specs=pl.BlockSpec(memory_space=pltpu.VMEM),
        scratch_shapes=[
            pltpu.VMEM((2, HALF, 4096), bf16),
            pltpu.VMEM((SIDE, 4096, 256), bf16),
            pltpu.VMEM((SIDE, FIELDS, 256, 256), bf16),
            pltpu.VMEM((SIDE, FIELDS, 256, 256), bf16),
            pltpu.VMEM((SIDE, FIELDS, 256, 256), bf16),
            pltpu.VMEM((SIDE, FIELDS, 256, BLK), bf16),
            pltpu.VMEM((chips, SIDE, FIELDS, 16, BLK), bf16),
            pltpu.VMEM((FIELDS, 256, BLK), bf16),
            pltpu.VMEM((SIDE, FIELDS, 16, BLK), bf16),
            pltpu.VMEM((chips, FIELDS, 16, BLK), bf16),
            pltpu.VMEM((SIDE - 1, FIELDS, 16, BLK), bf16),
            dma((2, 32)), dma((SIDE,)), dma((SIDE,)), dma((SIDE,)), dma((SIDE,)), dma((SIDE,)),
            dma((chips, SIDE)), dma((chips, SIDE)), dma((chips,)), dma((chips,)),
            dma((SIDE - 1,)), dma((SIDE - 1,)),
        ],
        compiler_params=pltpu.CompilerParams(
            collective_id=1, has_side_effects=True, vmem_limit_bytes=50 * 2**20
        ),
        cost_estimate=pl.CostEstimate(
            flops=30_000_000_000, bytes_accessed=30_000_000, transcendentals=0
        ),
    )(left, vir)


def body(
    dens_tiles,
    tile_dest,
    tile_place,
    tile_rows,
    tile_cols,
    ao_values,
    point_count,
    weights,
    kernel_first,
    kernel_second,
    occ_coef,
    vir_coef,
):
    ao = ao_values.reshape(NBAT * KB, BLK, PTS)
    dens, codes, occ_all = dispatch(
        tile_dest.T, tile_place.T, tile_rows, tile_cols,
        dens_tiles.reshape(TILES, ROWS, BLK), ao, occ_coef,
    )
    left = respond(
        codes, point_count, dens, weights, kernel_first, kernel_second, ao,
        occ_all,
    )
    return reduced(left, vir_coef)


def solution(mesh):
    in_specs = (
        P(("wide", "narrow"), None, None, None),
        P(("wide", "narrow"), None),
        P(("wide", "narrow"), None),
        P(("wide", "narrow")),
        P(("wide", "narrow")),
        P("wide", None, None),
        P("wide"),
        P("wide", None),
        P("wide", None),
        P("wide", None),
        P("wide", None),
        P("narrow", None),
    )
    out_specs = P(None, "wide", "narrow")
    return jax.shard_map(body, mesh=mesh, in_specs=in_specs, out_specs=out_specs, check_vma=False)
```

```python
import jax
import jax.numpy as jnp
from jax import lax
from jax.experimental import pallas as pl
from jax.experimental.pallas import tpu as pltpu
from jax.sharding import PartitionSpec as P

NOCC = 512
NVIR = 1024
BLK = 128
KB = 5
FIELDS = 3
NBAT = 2
PTS = 1280
SIDE = 4
NWIDE = 32
TILES = 16
SLOTS = 8
ROWS = FIELDS * BLK
HALF = FIELDS * NOCC // 2
MESH = pl.DeviceIdType.MESH
CHIPS = [(2, 2), (1, 1), (3, 3), (1, 3), (3, 1), (1, 2), (3, 2), (2, 1), (2, 3), (0, 2), (2, 0), (0, 1), (0, 3), (1, 0), (3, 0)]
OUT_AHEAD, TILES_AHEAD, ON_AHEAD = 11, 8, 7
OFFSETS = [(z, x, c) for z, x in CHIPS for c in range(2)] + [(0, 0, 1)]


def shifted(me, offset, sign=1):
    z, x, c = me // 8, (me // 2) % 4, me % 2
    z = (z + sign * offset[0] + 2 * SIDE) % SIDE
    x = (x + sign * offset[1] + 2 * SIDE) % SIDE
    c = (c + offset[2]) % 2
    return z * 8 + x * 2 + c


def dispatch_kernel(
    dest_ref, place_ref, rows_ref, cols_ref, tiles_hbm, ao_hbm, occ_hbm, dens_ref, codes_ref, all_ref,
    tiles_ref, ao_ref, occ_ref, load_sem, meta_ref, info_ref, outb, inb, acc, mine, parts, block,
    send_sem, recv_sem, meta_send, meta_recv, part_send, part_recv,
    own_sem, plane_send, plane_recv, side_send, side_recv, pass_send, pass_recv, pair_send, pair_recv,
):
    me = lax.axis_index("wide")
    row = lax.axis_index("narrow")
    quarter = pl.ds(pl.multiple_of(row * BLK, BLK), BLK)
    load_occ = pltpu.make_async_copy(occ_hbm.at[quarter], occ_ref, load_sem.at[0])
    load_tiles = pltpu.make_async_copy(tiles_hbm, tiles_ref, load_sem.at[1])
    load_ao = pltpu.make_async_copy(ao_hbm, ao_ref, load_sem.at[2])
    load_occ.start()
    load_tiles.start()
    load_ao.start()
    barrier = pltpu.get_barrier_semaphore()
    for offset in OFFSETS:
        pl.semaphore_signal(
            barrier, inc=1, device_id={"wide": shifted(me, offset)}, device_id_type=MESH
        )
    for step in range(1, SIDE):
        pl.semaphore_signal(
            barrier, inc=1, device_id={"narrow": (row + step) % SIDE}, device_id_type=MESH
        )

    load_occ.wait()
    turned = occ_ref[...].T
    for w in range(NWIDE):
        block[pl.ds((w % 2) * 256 + (w // 2) * 16, 16), :] = turned[w * 16 : (w + 1) * 16]

    acc[...] = jnp.zeros_like(acc)
    pl.semaphore_wait(barrier, len(OFFSETS) + SIDE - 1)

    def step_of(k):
        dz = sum(jnp.where(k == n + 1, z, 0) for n, (z, _) in enumerate(CHIPS))
        dx = sum(jnp.where(k == n + 1, x, 0) for n, (_, x) in enumerate(CHIPS))
        return dz, dx

    core = me % 2

    def turn(k):
        d, e = k % 4, k // 4
        return e + core * (d - e), d + core * (e - d)

    def home_of(k):
        return shifted(me, (*turn(k), 0), -1)

    def slot(k, c, j, peer, source):
        return pltpu.make_async_remote_copy(
            src_ref=outb.at[2 * peer + j], dst_ref=inb.at[2 * source + j],
            send_sem=send_sem.at[2 * k + c, j], recv_sem=recv_sem.at[2 * k + c, j],
            device_id={"wide": peer}, device_id_type=MESH,
        )

    def info(k, peer, source):
        return pltpu.make_async_remote_copy(
            src_ref=meta_ref.at[peer], dst_ref=info_ref.at[source], send_sem=meta_send.at[k],
            recv_sem=meta_recv.at[k], device_id={"wide": peer}, device_id_type=MESH,
        )

    def send_tiles(k):
        dz, dx = step_of(k)
        for c in range(2):
            info(2 * k + c, shifted(me, (dz, dx, c)), me).start()
            for j in range(2):
                slot(k, c, j, shifted(me, (dz, dx, c)), me).start()

    def place(home, y):
        return all_ref.at[home * SIDE + (y + 2 * SIDE) % SIDE]

    def plane(k, peer, home, src=block):
        return pltpu.make_async_remote_copy(
            src_ref=src, dst_ref=place(home, row), send_sem=plane_send.at[k],
            recv_sem=plane_recv.at[k], device_id={"wide": peer}, device_id_type=MESH,
        )

    def send_block(k):
        plane(k, shifted(me, (*turn(k), 0)), me).start()

    def spread(src, k, home, side, way):
        return pltpu.make_async_remote_copy(
            src_ref=src, dst_ref=place(home, row), send_sem=side_send.at[k, side],
            recv_sem=side_recv.at[k, side], device_id={"narrow": (row + way + SIDE) % SIDE},
            device_id_type=MESH,
        )

    def passed(k, home, y, way):
        return pltpu.make_async_remote_copy(
            src_ref=place(home, y), dst_ref=place(home, y), send_sem=pass_send.at[k],
            recv_sem=pass_recv.at[k], device_id={"narrow": (row + way + SIDE) % SIDE},
            device_id_type=MESH,
        )

    def paired(k, home):
        four = all_ref.at[pl.ds(home * SIDE, SIDE)]
        return pltpu.make_async_remote_copy(
            src_ref=four, dst_ref=four, send_sem=pair_send.at[k], recv_sem=pair_recv.at[k],
            device_id={"wide": shifted(me, (0, 0, 1))}, device_id_type=MESH,
        )

    def outward(k):
        home = home_of(k)
        plane(k, home, home).wait_recv()
        for side, way in enumerate((1, -1)):
            spread(place(home, row), k, home, side, way).start()

    def forward(k):
        home = home_of(k)
        for e in range(1, SIDE):
            plane(
                4 * e + k, shifted(me, (*turn(4 * e), 0)), home, place(home, row)
            ).start()

    def onward(k):
        home = home_of(k)
        for side, way in enumerate((1, -1)):
            pltpu.make_async_remote_copy(
                src_ref=block, dst_ref=place(home, row - way), send_sem=side_send.at[k, side],
                recv_sem=side_recv.at[k, side], device_id={"narrow": (row - way + SIDE) % SIDE},
                device_id_type=MESH,
            ).wait_recv()
        way = 1 - 2 * (k % 2)
        passed(k, home, row - way, way).start()

    def across(k):
        home = home_of(k)
        passed(k, home, row + 2, 1).wait_recv()
        paired(k, home).start()

    def each(first, last, step):
        def run(k, carry):
            step(k)
            return carry

        lax.fori_loop(first, last, run, 0)

    keep = pltpu.make_async_copy(block, place(me, row), own_sem)
    keep.start()
    for side, way in enumerate((1, -1)):
        spread(block, 0, me, side, way).start()
    pair = shifted(me, (0, 0, 1))
    for k in (1, 2, 3, 4, 8, 12):
        send_block(k)
    load_tiles.wait()
    lane = lax.broadcasted_iota(jnp.int32, (8, BLK), 1)

    def route(peer):
        found = [-1, -1]
        for r in range(2 * TILES):
            hit = dest_ref[r % 2, r // 2] == peer
            found = [
                jnp.where(jnp.logical_and(hit, found[0] < 0), r, found[0]),
                jnp.where(jnp.logical_and(hit, found[0] >= 0), r, found[1]),
            ]
        codes = []
        for j in range(2):
            r = jnp.maximum(found[j], 0)
            t = r // 2
            spot = place_ref[r % 2, t]
            batch, block_pair = spot // 25, spot % 25
            code = (
                (batch * KB + block_pair // KB) + 16 * (batch * KB + block_pair % KB) + 256 * batch
                + 512 * spot + 32768 + 65536 * rows_ref[t] + 262144 * cols_ref[t]
            )
            codes.append(jnp.where(found[j] >= 0, code, 0))
            outb[2 * peer + j] = tiles_ref[t]
        meta_ref[peer] = jnp.where(lane == 0, codes[0], jnp.where(lane == 1, codes[1], 0))

    def route_chip(k):
        dz, dx = step_of(k)
        for c in range(2):
            route(shifted(me, (dz, dx, c)))

    def advance(k):
        pl.when(k < 15)(lambda: route_chip(k + 1))
        send_tiles(k)

    route(pair)
    route(me)
    route_chip(1)
    info(1, pair, me).start()
    for j in range(2):
        slot(0, 1, j, pair, me).start()
    advance(1)

    def relay(k):
        outward(k)
        forward(k)

    each(1, SIDE, relay)
    each(2, 1 + TILES_AHEAD, advance)

    def use(tile, code):
        first, second = code % 16, (code // 16) % 16
        batch, valid = (code // 256) % 2, (code // 32768) % 2
        lives = [jnp.logical_and(valid == 1, batch == b) for b in range(NBAT)]
        for q in range(PTS // 256):
            cols = pl.ds(q * 256, 256)
            mixed = jnp.dot(tile, ao_ref[second, :, cols], preferred_element_type=jnp.float32)
            left = ao_ref[first, :, cols].astype(jnp.float32)
            part = jnp.sum(
                mixed.reshape(FIELDS, BLK // 8, 8, 256) * left.reshape(1, BLK // 8, 8, 256), axis=1
            )
            for b in range(NBAT):
                acc[b, :, :, cols] += jnp.where(lives[b], part, 0.0)

    def code_of(ref, source, j):
        return ref[source, 0:1, j : j + 1][0, 0]

    load_ao.wait()
    for j in range(2):
        code = code_of(meta_ref, me, j)
        codes_ref[2 * me + j] = code
        use(outb[2 * me + j], code)

    def take(k, c, source):
        info(2 * k + c, source, source).wait_recv()
        for j in range(2):
            slot(k, c, j, source, source).wait_recv()
            code = code_of(info_ref, source, j)
            codes_ref[2 * source + j] = code
            use(inb[2 * source + j], code)

    take(0, 1, pair)
    keep.wait()
    each(SIDE, 1 + OUT_AHEAD, outward)
    each(0, 1 + ON_AHEAD, onward)
    across(0)

    def arrive(k):
        pl.when(k + TILES_AHEAD <= 15)(lambda: advance(k + TILES_AHEAD))
        pl.when(k + OUT_AHEAD <= 15)(lambda: outward(k + OUT_AHEAD))
        dz, dx = step_of(k)
        for c in range(2):
            take(k, c, shifted(me, (dz, dx, c), -1))
        pl.when(k + ON_AHEAD <= 15)(lambda: onward(k + ON_AHEAD))
        across(k)

    each(1, 16, arrive)

    for b in range(NBAT):
        for f in range(FIELDS):
            mine[pl.ds(b * FIELDS + f, 1), :] = jnp.sum(acc[b, f], axis=0, keepdims=True)
    mine[pl.ds(6, 2), :] = jnp.zeros((2, PTS), jnp.float32)
    total = mine[...]
    swaps = []
    for step in range(1, SIDE):
        copy = pltpu.make_async_remote_copy(
            src_ref=mine, dst_ref=parts.at[step - 1], send_sem=part_send.at[step - 1],
            recv_sem=part_recv.at[step - 1], device_id={"narrow": (row + step) % SIDE},
            device_id_type=MESH,
        )
        copy.start()
        swaps.append(copy)
    info(1, pair, me).wait_send()
    for j in range(2):
        slot(0, 1, j, pair, me).wait_send()

    def drain(k):
        plane(k, pair, me).wait_send()
        for c in range(2):
            info(2 * k + c, pair, me).wait_send()
            for j in range(2):
                slot(k, c, j, pair, me).wait_send()

    def finish(k):
        home = home_of(k)
        for side, way in enumerate((1, -1)):
            spread(block, k, home, side, way).wait_send()
        passed(k, home, row, 1).wait_send()
        paired(k, home).wait_send()
        dz, dx = turn(k)
        paired(k, shifted(me, (dx, dz, 1), -1)).wait_recv()

    each(1, 16, drain)
    each(0, 16, finish)
    for step, copy in enumerate(swaps):
        copy.wait()
        total = total + parts[step]
    dens_ref[...] = total


def dispatch(dest, place, rows, cols, tiles, ao, occ):
    vmem, smem = pl.BlockSpec(memory_space=pltpu.VMEM), pl.BlockSpec(memory_space=pltpu.SMEM)
    dma, hbm = pltpu.SemaphoreType.DMA, pl.BlockSpec(memory_space=pltpu.HBM)
    return pl.pallas_call(
        dispatch_kernel,
        out_shape=(
            jax.ShapeDtypeStruct((8, PTS), jnp.float32),
            jax.ShapeDtypeStruct((2 * NWIDE,), jnp.int32),
            jax.ShapeDtypeStruct((NWIDE * SIDE, NOCC, BLK), jnp.bfloat16),
        ),
        in_specs=[smem, smem, smem, smem, hbm, hbm, hbm],
        out_specs=(vmem, smem, hbm),
        scratch_shapes=[
            pltpu.VMEM((TILES, ROWS, BLK), jnp.bfloat16),
            pltpu.VMEM((NBAT * KB, BLK, PTS), jnp.bfloat16),
            pltpu.VMEM((BLK, NOCC), jnp.bfloat16),
            dma((3,)),
            pltpu.VMEM((NWIDE, 8, BLK), jnp.int32),
            pltpu.VMEM((NWIDE, 8, BLK), jnp.int32),
            pltpu.VMEM((2 * NWIDE, ROWS, BLK), jnp.bfloat16),
            pltpu.VMEM((2 * NWIDE, ROWS, BLK), jnp.bfloat16),
            pltpu.VMEM((NBAT, FIELDS, 8, PTS), jnp.float32),
            pltpu.VMEM((8, PTS), jnp.float32),
            pltpu.VMEM((SIDE - 1, 8, PTS), jnp.float32),
            pltpu.VMEM((NOCC, BLK), jnp.bfloat16),
            dma((NWIDE, 2)), dma((NWIDE, 2)),
            dma((NWIDE,)), dma((NWIDE,)), dma((SIDE - 1,)), dma((SIDE - 1,)),
            dma, dma((16,)), dma((16,)), dma((16, 2)), dma((16, 2)), dma((16,)), dma((16,)),
            dma((16,)), dma((16,)),
        ],
        compiler_params=pltpu.CompilerParams(
            collective_id=0, has_side_effects=True, vmem_limit_bytes=56 * 2**20
        ),
        cost_estimate=pl.CostEstimate(
            flops=70_000_000_000, bytes_accessed=10_000_000, transcendentals=0
        ),
    )(dest, place, rows, cols, tiles, ao, occ)


def respond_kernel(
    code_ref, count_ref, dens_ref, weight_ref, first_ref, second_ref, ao_ref, occ_hbm,
    left_hbm, occ, pot, scaled, answer, total, left, head, follow, occ_sem, left_sem,
):
    loads = [
        pltpu.make_async_copy(occ_hbm.at[pl.ds(i * 8, 8)], occ.at[pl.ds(i * 8, 8)], occ_sem.at[i])
        for i in range(16)
    ]
    for load in loads:
        load.start()

    lane = lax.broadcasted_iota(jnp.int32, (1, PTS), 1)
    for b in range(NBAT):
        scale = jnp.where(lane < count_ref[b], weight_ref[pl.ds(b, 1), :], 0.0)
        one, two = first_ref[pl.ds(b, 1), :], second_ref[pl.ds(b, 1), :]
        d = [dens_ref[pl.ds(b * FIELDS + f, 1), :] for f in range(FIELDS)]
        for f in range(FIELDS):
            p, q = d[(f + 1) % 3], d[(f + 2) % 3]
            pot[pl.ds(b * FIELDS + f, 1), :] = scale * (one * d[f] + two * p * q)

    def blocks(i, carry):
        b, f = i // FIELDS, i % FIELDS
        aos = ao_ref[pl.ds(b * KB, KB)].reshape(KB * BLK, PTS)
        scaled[...] = (aos.astype(jnp.float32) * pot[pl.ds(i, 1), :]).astype(jnp.bfloat16)
        part = lax.dot_general(
            scaled[...], aos, (((1,), (1,)), ((), ())), preferred_element_type=jnp.float32
        ).astype(jnp.bfloat16)
        for a in range(KB):
            for c in range(KB):
                answer[b * 25 + a * KB + c, :, pl.ds(pl.multiple_of(f * BLK, BLK), BLK)] = part[
                    a * BLK : (a + 1) * BLK, c * BLK : (c + 1) * BLK
                ]
        return carry

    lax.fori_loop(0, NBAT * FIELDS, blocks, 0)

    def clear(c, carry):
        head[c] = -1
        follow[2 * c] = -1
        follow[2 * c + 1] = -1
        return carry

    lax.fori_loop(0, 32, clear, 0)

    def link(r, carry):
        code = code_ref[r]
        column = (code // 262144) % 32

        @pl.when((code // 32768) % 2 == 1)
        def _():
            follow[r] = head[column]
            head[column] = r

        return carry

    lax.fori_loop(0, 2 * NWIDE, link, 0)
    for load in loads:
        load.wait()

    def column_sum(c, carry):
        def term(r):
            code = code_ref[r]
            return occ[(r // 2) * 4 + (code // 65536) % 4], answer[(code // 512) % 64]

        def two(r):
            nxt = follow[r]
            other = jnp.where(nxt >= 0, nxt, r)
            (left_a, right_a), (left_b, right_b) = term(r), term(other)
            right_b = jnp.where(nxt >= 0, right_b, jnp.zeros_like(right_b))
            return jnp.dot(
                jnp.concatenate([left_a, left_b], axis=1),
                jnp.concatenate([right_a, right_b], axis=0), preferred_element_type=jnp.float32,
            )

        def after(r):
            nxt = follow[jnp.maximum(r, 0)]
            last = jnp.logical_or(r < 0, nxt < 0)
            return jnp.where(last, -1, follow[jnp.maximum(nxt, 0)])

        def add(r):
            total[...] += two(r)
            return after(r)

        slot = c % SLOTS

        @pl.when(c >= SLOTS)
        def _():
            pltpu.make_async_copy(left.at[slot], left_hbm.at[c], left_sem.at[slot]).wait()

        def emit(value):
            value = value.astype(jnp.bfloat16)
            for half in range(2):
                for f in range(FIELDS):
                    left[slot, pl.ds(half * HALF + f * 256, 256), :] = value[
                        half * 256 : (half + 1) * 256, f * BLK : (f + 1) * BLK
                    ]

        first = head[c]
        second = after(first)

        @pl.when(first < 0)
        def _():
            left[slot] = jnp.zeros((2 * HALF, BLK), jnp.bfloat16)

        @pl.when(jnp.logical_and(first >= 0, second < 0))
        def _():
            emit(two(first))

        @pl.when(second >= 0)
        def _():
            total[...] = two(first)
            lax.while_loop(lambda r: r >= 0, add, second)
            emit(total[...])

        pltpu.make_async_copy(left.at[slot], left_hbm.at[c], left_sem.at[slot]).start()
        return carry

    lax.fori_loop(0, 32, column_sum, 0)
    for slot in range(SLOTS):
        pltpu.make_async_copy(left.at[slot], left_hbm.at[slot], left_sem.at[slot]).wait()


def respond(codes, counts, dens, weights, first, second, ao, occ):
    vmem, smem = pl.BlockSpec(memory_space=pltpu.VMEM), pl.BlockSpec(memory_space=pltpu.SMEM)
    hbm = pl.BlockSpec(memory_space=pltpu.HBM)
    return pl.pallas_call(
        respond_kernel,
        out_shape=jax.ShapeDtypeStruct((32, 2 * HALF, BLK), jnp.bfloat16),
        in_specs=[smem, smem, vmem, vmem, vmem, vmem, vmem, hbm],
        out_specs=hbm,
        scratch_shapes=[
            pltpu.VMEM((128, NOCC, BLK), jnp.bfloat16),
            pltpu.VMEM((8, PTS), jnp.float32),
            pltpu.VMEM((KB * BLK, PTS), jnp.bfloat16),
            pltpu.VMEM((50, BLK, ROWS), jnp.bfloat16),
            pltpu.VMEM((NOCC, ROWS), jnp.float32),
            pltpu.VMEM((SLOTS, 2 * HALF, BLK), jnp.bfloat16),
            pltpu.SMEM((32,), jnp.int32),
            pltpu.SMEM((64,), jnp.int32),
            pltpu.SemaphoreType.DMA((16,)),
            pltpu.SemaphoreType.DMA((SLOTS,)),
        ],
        compiler_params=pltpu.CompilerParams(vmem_limit_bytes=62 * 2**20),
        cost_estimate=pl.CostEstimate(
            flops=30_000_000_000, bytes_accessed=30_000_000, transcendentals=0
        ),
    )(codes, counts, dens, weights, first, second, ao, occ)


def reduce_kernel(
    left_hbm, vir_hbm, out_ref, left, vir, give, got, mid, y_one, x_one, y_sum, x_sum, x_two, y_two,
    left_sem, vir_sem, give_send, give_recv, y_one_send, y_one_recv, x_one_send, x_one_recv,
    x_two_send, x_two_recv, y_two_send, y_two_recv,
):
    me = lax.axis_index("wide")
    row = lax.axis_index("narrow")
    core, chip = me % 2, me // 2
    pair = shifted(me, (0, 0, 1))
    peers = [shifted(me, (z, x, 0)) for z, x in CHIPS]
    barrier = pltpu.get_barrier_semaphore()
    for peer in [pair, *peers]:
        pl.semaphore_signal(barrier, inc=1, device_id={"wide": peer}, device_id_type=MESH)
    for step in range(1, SIDE):
        pl.semaphore_signal(
            barrier, inc=1, device_id={"narrow": (row + step) % SIDE}, device_id_type=MESH
        )

    def load(half, c):
        rows = pl.ds(pl.multiple_of(half * HALF, HALF), HALF)
        return pltpu.make_async_copy(
            left_hbm.at[c, rows],
            left.at[half, :, pl.ds(pl.multiple_of(c * BLK, BLK), BLK)],
            left_sem.at[half, c],
        )

    def load_vir(q):
        return pltpu.make_async_copy(
            vir_hbm.at[:, pl.ds(pl.multiple_of(q * 256, 256), 256)], vir.at[q], vir_sem.at[q]
        )

    def each(last, step):
        def run(k, carry):
            step(k)
            return carry

        lax.fori_loop(0, last, run, 0)

    order = [(row + 1 + i) % SIDE for i in range(SIDE)]
    load_vir(order[0]).start()
    each(32, lambda c: load(1 - core, c).start())
    load_vir(order[1]).start()
    each(32, lambda c: load(core, c).start())
    for q in order[2:]:
        load_vir(q).start()
    pl.semaphore_wait(barrier, 1 + len(peers) + SIDE - 1)

    def to(axis, peer, src, dst, ssem, rsem):
        return pltpu.make_async_remote_copy(
            src_ref=src, dst_ref=dst, send_sem=ssem, recv_sem=rsem, device_id={axis: peer},
            device_id_type=MESH,
        )

    def product(half, q):
        return jnp.dot(left[half], vir[q], preferred_element_type=jnp.float32).reshape(
            FIELDS, 256, 256
        )

    def hand(q):
        return to("wide", pair, give.at[q], got.at[q], give_send.at[q], give_recv.at[q])

    def other_half(q):
        load_vir(q).wait()
        give[q] = product(1 - core, q).astype(jnp.bfloat16)
        hand(q).start()

    def down(q, y):
        return to(
            "narrow", q, mid.at[q, :, :, pl.ds(0, BLK)], y_one.at[y], y_one_send.at[q],
            y_one_recv.at[y],
        )

    def over(q, k, peer):
        rows = pl.ds(pl.multiple_of((peer // 2) * 16, 16), 16)
        return to(
            "wide", peer, mid.at[q, :, rows, pl.ds(BLK, BLK)], x_one.at[k, q],
            x_one_send.at[k, q], x_one_recv.at[k, q],
        )

    def own_half(q):
        own = product(core, q)
        hand(q).wait_recv()
        mid[q] = (own + got[q].astype(jnp.float32)).astype(jnp.bfloat16)
        pl.when(q != row)(lambda: down(q, row).start())
        for k, peer in enumerate(peers):
            over(q, k, peer).start()

    each(32, lambda c: load(1 - core, c).wait())
    other_half(order[0])
    each(32, lambda c: load(core, c).wait())

    def both(i):
        pl.when(i < SIDE - 1)(lambda: other_half((row + 2 + i) % SIDE))
        own_half((row + 1 + i) % SIDE)

    each(SIDE, both)
    here = pl.ds(pl.multiple_of(chip * 16, 16), 16)

    total = mid[row, :, :, pl.ds(0, BLK)].astype(jnp.float32)
    for step in range(1, SIDE):
        y = (row + step) % SIDE
        down(y, y).wait_recv()
        total = total + y_one[y].astype(jnp.float32)
    y_sum[...] = total.astype(jnp.bfloat16)

    def scatter(k, peer):
        rows = pl.ds(pl.multiple_of((peer // 2) * 16, 16), 16)
        return to("wide", peer, y_sum.at[:, rows], x_two.at[k], x_two_send.at[k], x_two_recv.at[k])

    for k, peer in enumerate(peers):
        scatter(k, peer).start()

    total = mid[:, :, here, pl.ds(BLK, BLK)].astype(jnp.float32)
    for k, peer in enumerate(peers):
        for q in range(SIDE):
            over(q, k, peer).wait_recv()
        total = total + x_one[k].astype(jnp.float32)
    x_sum[...] = total.astype(jnp.bfloat16)

    def give_row(step):
        y = (row + step) % SIDE
        return to(
            "narrow", y, x_sum.at[y], y_two.at[step - 1], y_two_send.at[step - 1],
            y_two_recv.at[step - 1],
        )

    for step in range(1, SIDE):
        give_row(step).start()

    total = y_sum[:, here].astype(jnp.float32)
    for k, peer in enumerate(peers):
        scatter(k, peer).wait_recv()
        total = total + x_two[k].astype(jnp.float32)
    out_ref[:, :, pl.ds(0, BLK)] = total
    total = x_sum[row].astype(jnp.float32)
    for step in range(1, SIDE):
        give_row(step).wait_recv()
        total = total + y_two[step - 1].astype(jnp.float32)
    out_ref[:, :, pl.ds(BLK, BLK)] = total

    def sent(q):
        hand(q).wait_send()
        pl.when(q != row)(lambda: down(q, row).wait_send())
        for k, peer in enumerate(peers):
            over(q, k, peer).wait_send()

    each(SIDE, sent)
    for k, peer in enumerate(peers):
        scatter(k, peer).wait_send()
    for step in range(1, SIDE):
        give_row(step).wait_send()


def reduced(left, vir):
    hbm = pl.BlockSpec(memory_space=pltpu.HBM)
    dma, bf16 = pltpu.SemaphoreType.DMA, jnp.bfloat16
    chips = len(CHIPS)
    return pl.pallas_call(
        reduce_kernel,
        out_shape=jax.ShapeDtypeStruct((FIELDS, 16, 256), jnp.float32),
        in_specs=[hbm, hbm],
        out_specs=pl.BlockSpec(memory_space=pltpu.VMEM),
        scratch_shapes=[
            pltpu.VMEM((2, HALF, 4096), bf16),
            pltpu.VMEM((SIDE, 4096, 256), bf16),
            pltpu.VMEM((SIDE, FIELDS, 256, 256), bf16),
            pltpu.VMEM((SIDE, FIELDS, 256, 256), bf16),
            pltpu.VMEM((SIDE, FIELDS, 256, 256), bf16),
            pltpu.VMEM((SIDE, FIELDS, 256, BLK), bf16),
            pltpu.VMEM((chips, SIDE, FIELDS, 16, BLK), bf16),
            pltpu.VMEM((FIELDS, 256, BLK), bf16),
            pltpu.VMEM((SIDE, FIELDS, 16, BLK), bf16),
            pltpu.VMEM((chips, FIELDS, 16, BLK), bf16),
            pltpu.VMEM((SIDE - 1, FIELDS, 16, BLK), bf16),
            dma((2, 32)), dma((SIDE,)), dma((SIDE,)), dma((SIDE,)), dma((SIDE,)), dma((SIDE,)),
            dma((chips, SIDE)), dma((chips, SIDE)), dma((chips,)), dma((chips,)),
            dma((SIDE - 1,)), dma((SIDE - 1,)),
        ],
        compiler_params=pltpu.CompilerParams(
            collective_id=1, has_side_effects=True, vmem_limit_bytes=50 * 2**20
        ),
        cost_estimate=pl.CostEstimate(
            flops=30_000_000_000, bytes_accessed=30_000_000, transcendentals=0
        ),
    )(left, vir)


def body(
    dens_tiles,
    tile_dest,
    tile_place,
    tile_rows,
    tile_cols,
    ao_values,
    point_count,
    weights,
    kernel_first,
    kernel_second,
    occ_coef,
    vir_coef,
):
    ao = ao_values.reshape(NBAT * KB, BLK, PTS)
    dens, codes, occ_all = dispatch(
        tile_dest.T, tile_place.T, tile_rows, tile_cols,
        dens_tiles.reshape(TILES, ROWS, BLK), ao, occ_coef,
    )
    left = respond(
        codes, point_count, dens, weights, kernel_first, kernel_second, ao,
        occ_all,
    )
    return reduced(left, vir_coef)


def solution(mesh):
    in_specs = (
        P(("wide", "narrow"), None, None, None),
        P(("wide", "narrow"), None),
        P(("wide", "narrow"), None),
        P(("wide", "narrow")),
        P(("wide", "narrow")),
        P("wide", None, None),
        P("wide"),
        P("wide", None),
        P("wide", None),
        P("wide", None),
        P("wide", None),
        P("narrow", None),
    )
    out_specs = P(None, "wide", "narrow")
    return jax.shard_map(body, mesh=mesh, in_specs=in_specs, out_specs=out_specs, check_vma=False)
```
